32 devices in a mesh: scen: 8 (over y, x, core), col: 4 (over z).
Axes of the slice: x: 2, y: 2, z: 4, core: 2. Of those that a mesh axis runs over, the one named last changes fastest.
Arguments:
- tech: bfloat16 [32, 2048, 4096], P('scen', None, 'col'), may hold values from -0.046875 to 0.046875
- recourse: bfloat16 [32, 2048, 1024], P('scen', None, 'col'), may hold values from -0.125 to 0.125
- rhs: float32 [32, 32, 2048], P(None, 'scen'), may hold values from -6 to 6
- cost_first: float32 [4096], P('col'), may hold values from -6 to 6
- cost_second: float32 [32, 1024], P('scen', 'col'), may hold values from -6 to 6
- cone_id: int32 [32, 2048], P('scen'), may hold values from 0 to 127, never falling along the last dimension, each value on 1 to 64 neighbouring positions
Outputs:
- first_section: float32 [32, 4096], P(None, 'col')
- second_section: float32 [32, 32, 1024], P(None, 'scen', 'col')
- slack: float32 [32, 32, 2048], P(None, 'scen', 'col')
- dual: float32 [32, 32, 2048], P(None, 'scen', 'col')
The draws below stay inside these ranges and needn't reach their ends.
Inputs may be any that keep to these rules, and one draw needn't show every extreme that they name: Along the rows of a scenario cone_id never falls; a cone holds 1 to 64 rows.
All inputs are finite; a program needn't handle non-finite values.
Results may differ from the reference program's by a relative error of at most 0.014.
Values may be sent and summed in bfloat16 or wider, within the bound.
A program may use at most 128 MiB of HBM per device.

```python
import math
import jax
import jax.numpy as jnp
import numpy as np
from jax import lax

M = 2048
NX = 4096
NY = 1024
NCONE = 128
CONE_MOST = 64
BATCH = 32
ITERS = 3
CG_STEPS = 3
SCENS = 32


def steps_of(key, shape, cuts, least, top_value):
    def one(dim, parts):
        draws = jax.random.uniform(jax.random.fold_in(jax.random.fold_in(key, 6), dim), (parts,), jnp.float32, least / len(cuts), top_value / len(cuts))
        return jnp.repeat(jnp.exp(draws), shape[dim] // parts).reshape((-1,) + (1,) * (len(shape) - dim - 1))

    gain = one(*cuts[0])
    for cut in cuts[1:]:
        gain = gain * one(*cut)
    return gain


def split_up(count, total, reach, slope):
    loads = [(1 << 20) // math.isqrt(grade ** slope) + 1 for grade in range(2, count + 1)]
    spare, holding = total - reach - (count - 1), [1] * (count - 1)
    while spare > 0:
        candidates = [i for i in range(count - 1) if holding[i] < reach]
        whole, left = sum([loads[i] for i in candidates]), spare
        for i in candidates:
            more = min(reach - holding[i], max(1, left * loads[i] // whole), spare)
            holding[i] = holding[i] + more
            spare = spare - more
    return np.array([reach] + holding)


def uneven_parts(rng, number_of, total, limit, lean):
    if number_of == 2:
        one = jax.random.randint(rng, (), max(1, total - limit), min(limit, total - 1) + 1)
        return jnp.stack([one, total - one])
    tallies = jnp.asarray(split_up(number_of, total, limit, lean), jnp.int32)
    couples = (number_of - 1) // 2
    source_of, receiver = tallies[1:1 + 2 * couples:2], tallies[2:2 + 2 * couples:2]
    room = jnp.minimum(source_of - 1, limit - receiver)
    moved = jax.random.randint(jax.random.fold_in(rng, 1), (couples,), 0, 1 << 20) % (room + 1)
    tallies = tallies.at[1:1 + 2 * couples:2].set(source_of - moved).at[2:2 + 2 * couples:2].set(receiver + moved)
    return tallies[jax.random.permutation(jax.random.fold_in(rng, 2), number_of)]


def bell_draw(key, shape, spread, reach, split=(), dtype=jnp.bfloat16):
    loudness = steps_of(key, shape, split, -0.22, 0.18) if split else 1.0
    entries = jax.random.normal(key, shape, jnp.float32) * spread * loudness
    return jnp.minimum(jnp.maximum(entries, -reach), reach).astype(dtype)


def setup_inputs(seed: int = 0) -> dict:
    key_of = jax.random.split(jax.random.key(seed), 7)
    tech = bell_draw(key_of[0], (SCENS, M, NX), (SCENS * M // 4) ** -0.5, 0.046875, ((0, 8), (2, 4)))
    recourse = bell_draw(key_of[1], (SCENS, M, NY), M ** -0.5, 0.125, ((0, 8), (2, 4)))
    rhs = bell_draw(key_of[2], (BATCH, SCENS, M), 1.0, 6.0, ((1, 8),), jnp.float32)
    cost_first = bell_draw(key_of[3], (NX,), 1.0, 6.0, ((0, 4),), jnp.float32)
    cost_second = bell_draw(key_of[4], (SCENS, NY), 1.0, 6.0, ((0, 8), (1, 4)), jnp.float32)
    cone_id = jax.vmap(lambda own: jnp.searchsorted(jnp.cumsum(uneven_parts(own, NCONE, M, CONE_MOST, 2)), jnp.arange(M), side="right"))(jax.random.split(key_of[5], SCENS)).reshape((SCENS, M)).astype(jnp.int32)
    return dict(tech=tech, recourse=recourse, rhs=rhs, cost_first=cost_first, cost_second=cost_second, cone_id=cone_id)


HIGH = lax.Precision.HIGHEST

def cone_factors(lead, tail):
    norm_tail = jnp.sqrt(tail)
    inside = norm_tail <= lead
    polar = norm_tail <= -lead
    safe = jnp.where(norm_tail > 0.0, norm_tail, 1.0)
    middle = 0.5 * (lead + norm_tail)
    head = jnp.where(inside, lead, jnp.where(polar, 0.0, middle))
    scale = jnp.where(inside, 1.0, jnp.where(polar, 0.0, middle / safe))
    return (head, scale)

def reference(tech, recourse, rhs, cost_first, cost_second, cone_id):
    f32 = jnp.float32
    bf16 = jnp.bfloat16
    batch = rhs.shape[0]
    scen_count = tech.shape[0]
    rows = tech.shape[1]
    rhs_s = jnp.transpose(rhs, (1, 0, 2))
    starts = jnp.concatenate([jnp.ones((scen_count, 1), f32), (cone_id[:, 1:] != cone_id[:, :-1]).astype(f32)], axis=1)
    labels = lax.broadcasted_iota(jnp.int32, (1, 1, NCONE), 2)
    onehot = (cone_id[:, :, None] == labels).astype(f32)
    start_rows = starts[:, None, :]

    def project(values):
        lead = jnp.einsum('sbm,smc->sbc', values * start_rows, onehot, precision=HIGH)
        tail = jnp.einsum('sbm,smc->sbc', values * values * (1.0 - start_rows), onehot, precision=HIGH)
        head, scale = cone_factors(lead, tail)
        head_rows = jnp.einsum('sbc,smc->sbm', head, onehot, precision=HIGH)
        scale_rows = jnp.einsum('sbc,smc->sbm', scale, onehot, precision=HIGH)
        return start_rows * head_rows + (1.0 - start_rows) * values * scale_rows

    def forward(dir_first_bf, dir_second_bf):

        def single(args):
            tech_s, rec_s, dir_s = args
            return jnp.dot(dir_first_bf, tech_s.T, preferred_element_type=f32) + jnp.dot(dir_s, rec_s.T, preferred_element_type=f32)
        return lax.map(single, (tech, recourse, dir_second_bf))

    def adjoint(rows_bf):

        def single(carry, args):
            tech_s, rec_s, rows_s = args
            return (carry + jnp.dot(rows_s, tech_s, preferred_element_type=f32), jnp.dot(rows_s, rec_s, preferred_element_type=f32))
        return lax.scan(single, jnp.zeros((batch, tech.shape[2]), f32), (tech, recourse, rows_bf))

    def squares(first_vec, second_vec):
        return lax.optimization_barrier(jnp.sum(first_vec * first_vec, axis=1)) + lax.optimization_barrier(jnp.sum(second_vec * second_vec, axis=(0, 2)))
    first_sol = jnp.zeros((batch, tech.shape[2]), f32)
    second_sol = jnp.zeros((scen_count, batch, recourse.shape[2]), f32)
    slack = jnp.zeros((scen_count, batch, rows), f32)
    dual = jnp.zeros((scen_count, batch, rows), f32)
    image = jnp.zeros((scen_count, batch, rows), f32)
    for outer in range(ITERS):
        resid_rows = (rhs_s - slack - dual - image).astype(bf16)
        back_first, back_second = adjoint(resid_rows)
        res_first = back_first - cost_first[None, :]
        res_second = back_second - cost_second[:, None, :]
        res_norm = squares(res_first, res_second)
        dir_first, dir_second = (res_first, res_second)
        for step in range(CG_STEPS):
            image_step = forward(dir_first.astype(bf16), dir_second.astype(bf16))
            curv = squares(dir_first, dir_second) + lax.optimization_barrier(jnp.sum(image_step * image_step, axis=(0, 2)))
            alpha = res_norm / curv
            first_sol = first_sol + alpha[:, None] * dir_first
            second_sol = second_sol + alpha[None, :, None] * dir_second
            image = image + alpha[None, :, None] * image_step
            if step + 1 < CG_STEPS:
                back_first, back_second = adjoint(image_step.astype(bf16))
                res_first = res_first - alpha[:, None] * (dir_first + back_first)
                res_second = res_second - alpha[None, :, None] * (dir_second + back_second)
                new_norm = squares(res_first, res_second)
                ratio = new_norm / res_norm
                dir_first = res_first + ratio[:, None] * dir_first
                dir_second = res_second + ratio[None, :, None] * dir_second
                res_norm = new_norm
        slack = project(rhs_s - image - dual)
        dual = dual + image + slack - rhs_s
    return (first_sol, jnp.transpose(second_sol, (1, 0, 2)), jnp.transpose(slack, (1, 0, 2)), jnp.transpose(dual, (1, 0, 2)))
```

```python
import functools

import jax
import jax.numpy as jnp
from jax import lax
from jax.experimental import pallas as pl
from jax.experimental.pallas import tpu as pltpu
from jax.sharding import PartitionSpec as P

NCONE = 128
ITERS = 3
CG_STEPS = 3
LAG_A = 4
LAG_B = 8


HIGH = lax.Precision.HIGHEST


def cone_factors(lead, tail):
    norm_tail = jnp.sqrt(tail)
    inside = norm_tail <= lead
    polar = norm_tail <= -lead
    safe = jnp.where(norm_tail > 0.0, norm_tail, 1.0)
    middle = 0.5 * (lead + norm_tail)
    head = jnp.where(inside, lead, jnp.where(polar, 0.0, middle))
    scale = jnp.where(inside, 1.0, jnp.where(polar, 0.0, middle / safe))
    return (head, scale)


def body(tech, recourse, rhs, cost_first, cost_second, cone_id):
    f32 = jnp.float32
    bf16 = jnp.bfloat16
    n_scen = lax.axis_size("scen")
    n_col = lax.axis_size("col")
    batch = rhs.shape[0]
    scen_local = tech.shape[0]
    rows = tech.shape[1]
    first_cols = tech.shape[2]
    tech_flat = tech.reshape(scen_local * rows, first_cols)
    starts = jnp.concatenate(
        [jnp.ones((scen_local, 1), f32), (cone_id[:, 1:] != cone_id[:, :-1]).astype(f32)], axis=1
    )
    labels = lax.broadcasted_iota(jnp.int32, (1, 1, NCONE), 2)
    onehot = (cone_id[:, :, None] == labels).astype(f32)
    part_rows = rows // n_col
    row_start = lax.axis_index("col") * part_rows
    row_weight = 1.0 / n_col
    share_cols = first_cols // n_scen
    cost_here = lax.dynamic_slice_in_dim(
        cost_first, lax.axis_index("scen") * share_cols, share_cols, 0
    )
    first_weight = 1.0
    start_rows = starts[None]

    def couple(partial_value):
        return lax.psum_scatter(partial_value, "scen", scatter_dimension=1, tiled=True)

    def adjoint(rows_bf):
        first_part = jnp.dot(
            rows_bf.reshape(batch, scen_local * rows), tech_flat, preferred_element_type=f32
        )
        second_part = jnp.einsum("bsm,smk->bsk", rows_bf, recourse, preferred_element_type=f32)
        return (first_part, second_part)

    def local_squares(first_vec, second_vec):
        return first_weight * jnp.sum(first_vec * first_vec, axis=1) + jnp.sum(
            second_vec * second_vec, axis=(1, 2)
        )

    def total_norm(first_vec, second_vec):
        return lax.psum(local_squares(first_vec, second_vec), ("scen", "col"))

    here_rows = rhs.shape[2]
    first_sol = jnp.zeros((batch, share_cols), f32)
    second_sol = jnp.zeros((batch, scen_local, recourse.shape[2]), f32)
    slack = jnp.zeros((batch, scen_local, here_rows), f32)
    dual = jnp.zeros((batch, scen_local, here_rows), f32)
    image = jnp.zeros((batch, scen_local, here_rows), f32)
    for outer in range(ITERS):
        resid_rows = (rhs - slack - dual - image).astype(bf16)
        back_first, back_second = adjoint(resid_rows)
        res_first = couple(back_first) - cost_here[None, :]
        res_second = back_second - cost_second[None]
        res_norm = total_norm(res_first, res_second)
        dir_first, dir_second = (res_first, res_second)
        for step in range(CG_STEPS):
            dir_first_bf = lax.all_gather(dir_first.astype(bf16), "scen", axis=1, tiled=True)
            forward_partial_value = lax.dot_general(
                dir_first_bf, tech_flat, (((1,), (1,)), ((), ())), preferred_element_type=f32
            )
            forward_partial_value = forward_partial_value.reshape(batch, scen_local, rows)
            image_step = lax.psum(
                forward_partial_value
                + jnp.einsum(
                    "bsk,smk->bsm", dir_second.astype(bf16), recourse, preferred_element_type=f32
                ),
                "col",
            )
            curv_term = local_squares(dir_first, dir_second) + row_weight * jnp.sum(
                image_step * image_step, axis=(1, 2)
            )
            curv = lax.psum(curv_term, ("scen", "col"))
            alpha = res_norm / curv
            first_sol = first_sol + alpha[:, None] * dir_first
            second_sol = second_sol + alpha[:, None, None] * dir_second
            image = image + alpha[:, None, None] * image_step
            if step + 1 < CG_STEPS:
                back_first, back_second = adjoint(image_step.astype(bf16))
                res_first = res_first - alpha[:, None] * (dir_first + couple(back_first))
                res_second = res_second - alpha[:, None, None] * (dir_second + back_second)
                new_norm = total_norm(res_first, res_second)
                ratio = new_norm / res_norm
                dir_first = res_first + ratio[:, None] * dir_first
                dir_second = res_second + ratio[:, None, None] * dir_second
                res_norm = new_norm
        values = rhs - image - dual
        project_lead = jnp.einsum("bsm,smc->bsc", values * start_rows, onehot, precision=HIGH)
        project_tail = jnp.einsum(
            "bsm,smc->bsc", values * values * (1.0 - start_rows), onehot, precision=HIGH
        )
        project_lead, project_tail = (project_lead, project_tail)
        head, scale = cone_factors(project_lead, project_tail)
        head_rows = jnp.einsum("bsc,smc->bsm", head, onehot, precision=HIGH)
        scale_rows = jnp.einsum("bsc,smc->bsm", scale, onehot, precision=HIGH)
        slack = start_rows * head_rows + (1.0 - start_rows) * values * scale_rows
        dual = dual + image + slack - rhs
    first_out = lax.all_gather(first_sol, "scen", axis=1, tiled=True)
    slack_out = lax.dynamic_slice_in_dim(slack, row_start, part_rows, 2)
    dual_out = lax.dynamic_slice_in_dim(dual, row_start, part_rows, 2)
    return (first_out, second_sol, slack_out, dual_out)


def kernel_body(
    dims,
    tech_hbm, rec_hbm, rhs_hbm, cost1, cost2, cid, starts,
    x_out, y_out, slack_out, dual_out,
    wts, g, dual, slack, onehot, part, pb, rcv_a, rcv_b, q_own, q_all,
    acc, snd, rs1, ag1, back2, res2, dir2, res1, dir1,
    nrm_own, nrm1, nrm_mid, nrm2, crv_own, crv1, crv_mid, crv2,
    nres, ratio, alpha, qq, dq, xs,
    ld_t, ld_r, ld_g,
    ag1_s, ag1_r, n1_s, n1_r, n2_s, n2_r, a_s, a_r, b_s, b_r, q_s, q_r,
    c1_s, c1_r, c2_s, c2_r, rs1_s, rs1_r, fin_s, fin_r,
):
    n_scen, n_col, B, S, R, C1, C2 = dims
    f32, bf16 = jnp.float32, jnp.bfloat16
    H = n_col
    RH = R // H
    N = S * H
    SH = C1 // n_scen
    G = B // 8
    W = 128 // G
    ms = lax.axis_index("scen")
    mc = lax.axis_index("col")
    pair = mc + 1 - 2 * lax.rem(mc, 2)
    across = 3 - mc
    is_end = jnp.logical_or(mc == 0, mc == 3)
    is_mid = jnp.logical_or(mc == 1, mc == 2)

    def scen_peer(j):
        return lax.rem(ms + j, n_scen)

    def col_peer(j):
        return lax.rem(mc + j, n_col)

    def to_scen(src, dst, ss, rs, j):
        return pltpu.make_async_remote_copy(
            src_ref=src, dst_ref=dst, send_sem=ss, recv_sem=rs,
            device_id=(scen_peer(j), mc), device_id_type=pl.DeviceIdType.MESH)

    def to_col(src, dst, ss, rs, target):
        return pltpu.make_async_remote_copy(
            src_ref=src, dst_ref=dst, send_sem=ss, recv_sem=rs,
            device_id=(ms, target), device_id_type=pl.DeviceIdType.MESH)

    SJ = range(1, n_scen)
    CJ = range(1, n_col)

    def d_ag1(j):
        return to_scen(ag1.at[ms], ag1.at[ms], ag1_s.at[j - 1], ag1_r.at[j - 1], j)

    def d_n1(j):
        return to_scen(nrm_own, nrm1.at[j - 1], n1_s.at[j - 1], n1_r.at[j - 1], j)

    def d_n2(j):
        return to_col(nrm_mid, nrm2.at[j - 1], n2_s.at[j - 1], n2_r.at[j - 1], col_peer(j))

    def d_a(c):
        return to_col(pb.at[c], rcv_a.at[c], a_s.at[c], a_r.at[c], pair)

    def d_b(c):
        return to_col(pb.at[c], rcv_b.at[c], b_s.at[c], b_r.at[c], across)

    def d_q(c):
        return to_col(q_all.at[c], q_all.at[c], q_s.at[c], q_r.at[c], pair)

    def d_c1(j):
        return to_col(crv_own, crv1.at[j - 1], c1_s.at[j - 1], c1_r.at[j - 1], col_peer(j))

    def d_c2(j):
        return to_scen(crv_mid, crv2.at[j - 1], c2_s.at[j - 1], c2_r.at[j - 1], j)

    def d_rs1(j):
        return to_scen(snd.at[scen_peer(j)], rs1.at[j - 1], rs1_s.at[j - 1], rs1_r.at[j - 1], j)

    def d_fin(j):
        return to_scen(xs.at[ms], xs.at[ms], fin_s.at[j - 1], fin_r.at[j - 1], j)

    group = lax.broadcasted_iota(jnp.int32, (8, 128), 1) // W

    def pack(x):
        shift = 64
        while shift >= W:
            x = x + pltpu.roll(x, shift, 1)
            shift //= 2
        out = x[0:8]
        for k in range(1, G):
            out = jnp.where(group == k, x[8 * k:8 * k + 8], out)
        return out

    def unpack(p):
        return jnp.concatenate(
            [jnp.broadcast_to(jnp.sum(jnp.where(group == k, p, 0.0), axis=1, keepdims=True), (8, 128))
             for k in range(G)], axis=0)

    def lanes(x):
        out = x[:, 0:128]
        for k in range(1, x.shape[1] // 128):
            out = out + x[:, 128 * k:128 * k + 128]
        return out

    def rows_of(c):
        return c // H, pl.ds(pl.multiple_of(lax.rem(c, H) * RH, RH), RH)

    def load_t(c):
        s, rows = rows_of(c)
        return pltpu.make_async_copy(tech_hbm.at[s, rows, :], wts.at[c, :, pl.ds(0, C1)], ld_t.at[c])

    def load_r(c):
        s, rows = rows_of(c)
        return pltpu.make_async_copy(rec_hbm.at[s, rows, :], wts.at[c, :, pl.ds(C1, C2)], ld_r.at[c])

    def load_g(c):
        s, rows = rows_of(c)
        return pltpu.make_async_copy(rhs_hbm.at[s, :, rows], g.at[c], ld_g.at[c])

    def each(n, f):
        def one(c, carry):
            f(c)
            return carry
        lax.fori_loop(0, n, one, 0)

    each(N, lambda c: load_g(c).start())

    def load_w(c):
        load_t(c).start()
        load_r(c).start()

    each(N, load_w)

    barrier = pltpu.get_barrier_semaphore()
    for j in SJ:
        pl.semaphore_signal(barrier, inc=1, device_id=(scen_peer(j), mc), device_id_type=pl.DeviceIdType.MESH)
    for j in CJ:
        pl.semaphore_signal(barrier, inc=1, device_id=(ms, col_peer(j)), device_id_type=pl.DeviceIdType.MESH)

    dir1[...] = jnp.zeros_like(dir1)
    dir2[...] = jnp.zeros_like(dir2)
    q_own[...] = jnp.zeros_like(q_own)
    dual[...] = jnp.zeros_like(dual)
    xs[ms] = jnp.zeros((B, SH), f32)
    y_out[...] = jnp.zeros_like(y_out)

    def init(c):
        load_g(c).wait()
        q_all[c] = g[c].astype(bf16)

    each(N, init)

    def init_cones(s):
        ids = cid[pl.ds(s, 1), :]
        onehot[s] = (lax.broadcasted_iota(jnp.int32, (NCONE, R), 0) == ids).astype(f32).astype(bf16)

    each(S, init_cones)

    def clear_back():
        acc[...] = jnp.zeros_like(acc)
        back2[...] = jnp.zeros_like(back2)

    def back(c):
        s = c // H
        f = jnp.dot(q_all[c], wts[c], preferred_element_type=f32)
        for i in range(n_scen):
            acc[i] = acc[i] + f[:, i * SH:(i + 1) * SH]
        back2[s] = back2[s] + f[:, C1:C1 + C2]

    clear_back()

    def first_back(c):
        load_t(c).wait()
        load_r(c).wait()
        back(c)

    each(N, first_back)
    pl.semaphore_wait(barrier, n_scen + n_col - 2)

    def curv_forward():
        total = crv_own[...]
        for j in CJ:
            d_c1(j).wait_recv()
            total = total + crv1[j - 1]
        for j in CJ:
            d_c1(j).wait_send()
        crv_mid[...] = total
        for j in SJ:
            d_c2(j).start()

    def curv_finish():
        total = crv_mid[...]
        for j in SJ:
            d_c2(j).wait_recv()
            total = total + crv2[j - 1]
        for j in SJ:
            d_c2(j).wait_send()
        alpha[...] = nres[...] / unpack(total)

    def advance():
        a = alpha[...][:, 0:1]
        xs[ms] = xs[ms] + a * dir1[...]
        for s in range(S):
            y_out[s] = y_out[s] + a * dir2[s]

        def one(c):
            g[c] = g[c] - a * q_all[c].astype(f32)

        each(N, one)

    def split(x):
        hi = x.astype(bf16)
        return [hi, (x - hi.astype(f32)).astype(bf16)]

    def project(s):
        st = starts[pl.ds(s, 1), :]
        gs = jnp.concatenate([g[s * H + h] for h in range(H)], axis=1)
        v = gs - jnp.concatenate([dual[s * H + h] for h in range(H)], axis=1)
        lead_v = v * st
        tail_v = v * v * (1.0 - st)
        stack = jnp.concatenate(split(lead_v) + split(tail_v), axis=0)
        sums = lax.dot_general(stack, onehot[s], (((1,), (1,)), ((), ())), preferred_element_type=f32)
        lead = sums[0:B] + sums[B:2 * B]
        tail = sums[2 * B:3 * B] + sums[3 * B:4 * B]
        head, scale = cone_factors(lead, tail)
        stack2 = jnp.concatenate(split(head) + split(scale), axis=0)
        outs = jnp.dot(stack2, onehot[s], preferred_element_type=f32)
        head_rows = outs[0:B] + outs[B:2 * B]
        scale_rows = outs[2 * B:3 * B] + outs[3 * B:4 * B]
        sl = st * head_rows + (1.0 - st) * v * scale_rows
        du = sl - v
        d = (gs - sl - du).astype(bf16)
        for h in range(H):
            cols = slice(h * RH, (h + 1) * RH)
            slack[s * H + h] = sl[:, cols]
            dual[s * H + h] = du[:, cols]
            q_all[s * H + h] = d[:, cols]

    def norm_forward():
        total = nrm_own[...]
        for j in SJ:
            d_n1(j).wait_recv()
            total = total + nrm1[j - 1]
        for j in SJ:
            d_n1(j).wait_send()
        nrm_mid[...] = total
        for j in CJ:
            d_n2(j).start()

    def step_body(t, carry):
        step = lax.rem(t, CG_STEPS)
        last = step == CG_STEPS - 1
        for i in range(n_scen):
            snd[i] = acc[i].astype(bf16)
        for j in SJ:
            d_rs1(j).start()

        @pl.when(step != 0)
        def _():
            curv_forward()
            curv_finish()

        tot = acc[ms]
        for j in SJ:
            d_rs1(j).wait_recv()
            tot = tot + rs1[j - 1].astype(f32)

        @pl.when(step == 0)
        def _():
            res1[...] = tot - cost1[:, pl.ds(pl.multiple_of(ms * SH, 128), SH)]
            for s in range(S):
                res2[s] = back2[s] - cost2[s:s + 1, :]

        @pl.when(step != 0)
        def _():
            a = alpha[...][:, 0:1]
            res1[...] = res1[...] - a * (dir1[...] + tot)
            for s in range(S):
                res2[s] = res2[s] - a * (dir2[s] + back2[s])

        r1 = res1[...]
        ag1[ms] = r1.astype(bf16)
        for j in SJ:
            d_ag1(j).start()
        sq = lanes(r1 * r1)
        for s in range(S):
            r2 = res2[s]
            sq = sq + lanes(r2 * r2)
        nrm_own[...] = pack(sq)
        for j in SJ:
            d_n1(j).start()
        for j in SJ:
            d_rs1(j).wait_send()

        @pl.when(step != 0)
        def _():
            advance()

        clear_back()
        for j in SJ:
            d_ag1(j).wait_recv()
        for j in SJ:
            d_ag1(j).wait_send()

        def norm_finish():
            total = nrm_mid[...]
            for j in CJ:
                d_n2(j).wait_recv()
                total = total + nrm2[j - 1]
            for j in CJ:
                d_n2(j).wait_send()
            new = unpack(total)

            @pl.when(step == 0)
            def _():
                ratio[...] = jnp.zeros_like(ratio)

            @pl.when(step != 0)
            def _():
                ratio[...] = new / nres[...]

            nres[...] = new
            r = ratio[...][:, 0:1]
            d1 = res1[...] + r * dir1[...]
            dir1[...] = d1
            dsq = lanes(d1 * d1)
            for s in range(S):
                d2 = res2[s] + r * dir2[s]
                dir2[s] = d2
                dsq = dsq + lanes(d2 * d2)
            dq[...] = dsq

        def front(c):
            x = jnp.concatenate([ag1[i] for i in range(n_scen)] + [res2[c // H].astype(bf16)], axis=1)
            return lax.dot_general(x, wts[c], (((1,), (1,)), ((), ())), preferred_element_type=f32)

        def send_curv(sq):
            crv_own[...] = pack(sq)
            for j in CJ:
                d_c1(j).start()

        @pl.when(is_end)
        def _():
            def go(c):
                pb[c] = front(c).astype(bf16)
                d_a(c).start()

                @pl.when(c == 1)
                def _():
                    norm_forward()

            each(N, go)
            norm_finish()
            send_curv(dq[...])

            def take(c):
                d_q(c).wait_recv()

                @pl.when(jnp.logical_not(last))
                def _():
                    back(c)

            each(N, take)
            each(N, lambda c: d_a(c).wait_send())

        @pl.when(is_mid)
        def _():
            qq[...] = jnp.zeros_like(qq)

            def go(i):
                @pl.when(i < N)
                def _():
                    part[i] = front(i)

                @pl.when(i == 1)
                def _():
                    norm_forward()

                @pl.when(jnp.logical_and(i >= LAG_A, i < N + LAG_A))
                def _():
                    c = i - LAG_A
                    d_a(c).wait_recv()
                    pb[c] = (part[c] + rcv_a[c].astype(f32)).astype(bf16)
                    d_b(c).start()

                @pl.when(i == LAG_B)
                def _():
                    norm_finish()

                @pl.when(i >= LAG_B)
                def _():
                    c = i - LAG_B
                    r = ratio[...][:, 0:1]
                    d_b(c).wait_recv()
                    q = pb[c].astype(f32) + rcv_b[c].astype(f32) + r * q_own[c]
                    q_own[c] = q
                    q_all[c] = q.astype(bf16)
                    d_q(c).start()
                    qq[...] = qq[...] + lanes(q * q)

                    @pl.when(jnp.logical_not(last))
                    def _():
                        back(c)

            each(N + LAG_B, go)
            send_curv(dq[...] + 0.5 * qq[...])

            def sent(c):
                d_b(c).wait_send()
                d_q(c).wait_send()

            each(N, sent)

        @pl.when(last)
        def _():
            curv_forward()
            curv_finish()
            advance()
            each(S, project)

            @pl.when(t < ITERS * CG_STEPS - 1)
            def _():
                each(N, back)

        return carry

    lax.fori_loop(0, ITERS * CG_STEPS, step_body, 0)

    for j in SJ:
        d_fin(j).start()
    for s in range(S):
        slack_out[s] = slack[s * H + mc]
        dual_out[s] = dual[s * H + mc]
    for j in SJ:
        d_fin(j).wait_recv()
    for j in SJ:
        d_fin(j).wait_send()
    for i in range(n_scen):
        x_out[:, i * SH:(i + 1) * SH] = xs[i]


def fused(tech, recourse, rhs, cost_first, cost_second, cone_id):
    f32, bf16 = jnp.float32, jnp.bfloat16
    n_scen = lax.axis_size("scen")
    n_col = lax.axis_size("col")
    B = rhs.shape[0]
    S, R, C1 = tech.shape
    C2 = recourse.shape[2]
    RH = R // n_col
    N = S * n_col
    SH = C1 // n_scen
    starts = jnp.concatenate(
        [jnp.ones((S, 1), f32), (cone_id[:, 1:] != cone_id[:, :-1]).astype(f32)], axis=1)
    vm = pl.BlockSpec(memory_space=pltpu.VMEM)
    hbm = pl.BlockSpec(memory_space=pl.ANY)
    V = pltpu.VMEM
    D = pltpu.SemaphoreType.DMA
    ns, nc = n_scen - 1, n_col - 1
    rows = lambda dt: V((N, B, RH), dt)
    scratch = [
        V((N, RH, C1 + C2), bf16),
        rows(f32), rows(f32), rows(f32), V((S, NCONE, R), bf16),
        rows(f32), rows(bf16), rows(bf16), rows(bf16), rows(f32), rows(bf16),
        V((n_scen, B, SH), f32), V((n_scen, B, SH), bf16), V((ns, B, SH), bf16), V((n_scen, B, SH), bf16),
        V((S, B, C2), f32), V((S, B, C2), f32), V((S, B, C2), f32),
        V((B, SH), f32), V((B, SH), f32),
        V((8, 128), f32), V((ns, 8, 128), f32), V((8, 128), f32), V((nc, 8, 128), f32),
        V((8, 128), f32), V((nc, 8, 128), f32), V((8, 128), f32), V((ns, 8, 128), f32),
        V((B, 128), f32), V((B, 128), f32), V((B, 128), f32), V((B, 128), f32), V((B, 128), f32),
        V((n_scen, B, SH), f32),
        D((N,)), D((N,)), D((N,)),
        D((ns,)), D((ns,)), D((ns,)), D((ns,)), D((nc,)), D((nc,)),
        D((N,)), D((N,)), D((N,)), D((N,)), D((N,)), D((N,)),
        D((nc,)), D((nc,)), D((ns,)), D((ns,)), D((ns,)), D((ns,)), D((ns,)), D((ns,)),
    ]
    x, y, slack, dual = pl.pallas_call(
        functools.partial(kernel_body, (n_scen, n_col, B, S, R, C1, C2)),
        out_shape=(
            jax.ShapeDtypeStruct((B, C1), f32),
            jax.ShapeDtypeStruct((S, B, C2), f32),
            jax.ShapeDtypeStruct((S, B, RH), f32),
            jax.ShapeDtypeStruct((S, B, RH), f32),
        ),
        in_specs=[hbm, hbm, hbm, vm, vm, vm, vm],
        out_specs=(vm, vm, vm, vm),
        scratch_shapes=scratch,
        compiler_params=pltpu.CompilerParams(
            collective_id=0, has_side_effects=True, vmem_limit_bytes=58 * 1024 * 1024),
    )(
        tech, recourse, jnp.transpose(rhs, (1, 0, 2)),
        cost_first.reshape(1, C1), cost_second, cone_id, starts,
    )
    back = lambda a: jnp.transpose(a, (1, 0, 2))
    return x, back(y), back(slack), back(dual)


def program(tech, recourse, rhs, cost_first, cost_second, cone_id):
    n_scen = lax.axis_size("scen")
    n_col = lax.axis_size("col")
    batch = rhs.shape[0]
    fits = (
        tech.shape[2] % (128 * n_scen) == 0
        and tech.shape[1] % (128 * n_col) == 0
        and recourse.shape[2] % 128 == 0
        and batch % 16 == 0
        and 1024 % batch == 0
        and n_scen > 1
        and n_col == 4
    )
    run = fused if fits else body
    return run(tech, recourse, rhs, cost_first, cost_second, cone_id)


def solution(mesh):
    placed = (
        P("scen", None, "col"),
        P("scen", None, "col"),
        P(None, "scen", None),
        P("col"),
        P("scen", "col"),
        P("scen", None),
    )
    return jax.shard_map(
        program,
        mesh=mesh,
        in_specs=placed,
        out_specs=(
            P(None, "col"),
            P(None, "scen", "col"),
            P(None, "scen", "col"),
            P(None, "scen", "col"),
        ),
        check_vma=False,
    )
```

```python
import functools

import jax
import jax.numpy as jnp
from jax import lax
from jax.experimental import pallas as pl
from jax.experimental.pallas import tpu as pltpu
from jax.sharding import PartitionSpec as P

NCONE = 128
ITERS = 3
CG_STEPS = 3
CHUNKS = 2
LAG_A = 3
LAG_B = 6
LAG_E = 7


HIGH = lax.Precision.HIGHEST


def cone_factors(lead, tail):
    norm_tail = jnp.sqrt(tail)
    inside = norm_tail <= lead
    polar = norm_tail <= -lead
    safe = jnp.where(norm_tail > 0.0, norm_tail, 1.0)
    middle = 0.5 * (lead + norm_tail)
    head = jnp.where(inside, lead, jnp.where(polar, 0.0, middle))
    scale = jnp.where(inside, 1.0, jnp.where(polar, 0.0, middle / safe))
    return (head, scale)


def body(tech, recourse, rhs, cost_first, cost_second, cone_id):
    f32 = jnp.float32
    bf16 = jnp.bfloat16
    n_scen = lax.axis_size("scen")
    n_col = lax.axis_size("col")
    batch = rhs.shape[0]
    scen_local = tech.shape[0]
    rows = tech.shape[1]
    first_cols = tech.shape[2]
    tech_flat = tech.reshape(scen_local * rows, first_cols)
    starts = jnp.concatenate(
        [jnp.ones((scen_local, 1), f32), (cone_id[:, 1:] != cone_id[:, :-1]).astype(f32)], axis=1
    )
    labels = lax.broadcasted_iota(jnp.int32, (1, 1, NCONE), 2)
    onehot = (cone_id[:, :, None] == labels).astype(f32)
    part_rows = rows // n_col
    row_start = lax.axis_index("col") * part_rows
    row_weight = 1.0 / n_col
    share_cols = first_cols // n_scen
    cost_here = lax.dynamic_slice_in_dim(
        cost_first, lax.axis_index("scen") * share_cols, share_cols, 0
    )
    first_weight = 1.0
    start_rows = starts[None]

    def couple(partial_value):
        return lax.psum_scatter(partial_value, "scen", scatter_dimension=1, tiled=True)

    def adjoint(rows_bf):
        first_part = jnp.dot(
            rows_bf.reshape(batch, scen_local * rows), tech_flat, preferred_element_type=f32
        )
        second_part = jnp.einsum("bsm,smk->bsk", rows_bf, recourse, preferred_element_type=f32)
        return (first_part, second_part)

    def local_squares(first_vec, second_vec):
        return first_weight * jnp.sum(first_vec * first_vec, axis=1) + jnp.sum(
            second_vec * second_vec, axis=(1, 2)
        )

    def total_norm(first_vec, second_vec):
        return lax.psum(local_squares(first_vec, second_vec), ("scen", "col"))

    here_rows = rhs.shape[2]
    first_sol = jnp.zeros((batch, share_cols), f32)
    second_sol = jnp.zeros((batch, scen_local, recourse.shape[2]), f32)
    slack = jnp.zeros((batch, scen_local, here_rows), f32)
    dual = jnp.zeros((batch, scen_local, here_rows), f32)
    image = jnp.zeros((batch, scen_local, here_rows), f32)
    for outer in range(ITERS):
        resid_rows = (rhs - slack - dual - image).astype(bf16)
        back_first, back_second = adjoint(resid_rows)
        res_first = couple(back_first) - cost_here[None, :]
        res_second = back_second - cost_second[None]
        res_norm = total_norm(res_first, res_second)
        dir_first, dir_second = (res_first, res_second)
        for step in range(CG_STEPS):
            dir_first_bf = lax.all_gather(dir_first.astype(bf16), "scen", axis=1, tiled=True)
            forward_partial_value = lax.dot_general(
                dir_first_bf, tech_flat, (((1,), (1,)), ((), ())), preferred_element_type=f32
            )
            forward_partial_value = forward_partial_value.reshape(batch, scen_local, rows)
            image_step = lax.psum(
                forward_partial_value
                + jnp.einsum(
                    "bsk,smk->bsm", dir_second.astype(bf16), recourse, preferred_element_type=f32
                ),
                "col",
            )
            curv_term = local_squares(dir_first, dir_second) + row_weight * jnp.sum(
                image_step * image_step, axis=(1, 2)
            )
            curv = lax.psum(curv_term, ("scen", "col"))
            alpha = res_norm / curv
            first_sol = first_sol + alpha[:, None] * dir_first
            second_sol = second_sol + alpha[:, None, None] * dir_second
            image = image + alpha[:, None, None] * image_step
            if step + 1 < CG_STEPS:
                back_first, back_second = adjoint(image_step.astype(bf16))
                res_first = res_first - alpha[:, None] * (dir_first + couple(back_first))
                res_second = res_second - alpha[:, None, None] * (dir_second + back_second)
                new_norm = total_norm(res_first, res_second)
                ratio = new_norm / res_norm
                dir_first = res_first + ratio[:, None] * dir_first
                dir_second = res_second + ratio[:, None, None] * dir_second
                res_norm = new_norm
        values = rhs - image - dual
        project_lead = jnp.einsum("bsm,smc->bsc", values * start_rows, onehot, precision=HIGH)
        project_tail = jnp.einsum(
            "bsm,smc->bsc", values * values * (1.0 - start_rows), onehot, precision=HIGH
        )
        project_lead, project_tail = (project_lead, project_tail)
        head, scale = cone_factors(project_lead, project_tail)
        head_rows = jnp.einsum("bsc,smc->bsm", head, onehot, precision=HIGH)
        scale_rows = jnp.einsum("bsc,smc->bsm", scale, onehot, precision=HIGH)
        slack = start_rows * head_rows + (1.0 - start_rows) * values * scale_rows
        dual = dual + image + slack - rhs
    first_out = lax.all_gather(first_sol, "scen", axis=1, tiled=True)
    slack_out = lax.dynamic_slice_in_dim(slack, row_start, part_rows, 2)
    dual_out = lax.dynamic_slice_in_dim(dual, row_start, part_rows, 2)
    return (first_out, second_sol, slack_out, dual_out)


def kernel_body(
    dims,
    tech_hbm, rec_hbm, rhs_hbm, cost1, cost2, cid, starts,
    x_out, y_out, slack_out, dual_out,
    wts, wtt, g, dual, slack, onehot, part, pb, rcv_a, rcv_b, u, dz,
    px, acc, bq1, res1, dir1, sol1, xin, bk2, bq2, res2, dir2, sol2,
    sc1, sc2, uu, uv, uw,
    nres, dirn, qn, rat, alphas, rats,
    ld_t, ld_r, ld_g,
    a_s, a_r, b_s, b_r, u_s, u_r, px_s, px_r, c1_s, c1_r, c2_s, c2_r,
):
    n_scen, n_col, B, S, R, C1, C2 = dims
    f32, bf16 = jnp.float32, jnp.bfloat16
    H = CHUNKS
    RH = R // H
    N = S * H
    K = B // 2
    CB = 256
    G = K // 8
    W = 128 // (5 * G)
    TAIL = N // 2
    SLOTS = N + LAG_A
    TURNS = 2 * ITERS * (CG_STEPS + 1)
    ms = lax.axis_index("scen")
    mc = lax.axis_index("col")
    pair = mc + 1 - 2 * lax.rem(mc, 2)
    across = 3 - mc
    is_end = jnp.logical_or(mc == 0, mc == 3)
    is_mid = jnp.logical_or(mc == 1, mc == 2)
    lag = LAG_E - (LAG_E - LAG_B) * lax.rem((mc + 1) // 2, 2)

    def scen_peer(j):
        return lax.rem(ms + j, n_scen)

    def col_peer(j):
        return lax.rem(mc + j, n_col)

    def to_scen(src, dst, ss, rs, j):
        return pltpu.make_async_remote_copy(
            src_ref=src, dst_ref=dst, send_sem=ss, recv_sem=rs,
            device_id=(scen_peer(j), mc), device_id_type=pl.DeviceIdType.MESH)

    def to_col(src, dst, ss, rs, target):
        return pltpu.make_async_remote_copy(
            src_ref=src, dst_ref=dst, send_sem=ss, recv_sem=rs,
            device_id=(ms, target), device_id_type=pl.DeviceIdType.MESH)

    SJ = range(1, n_scen)
    CJ = range(1, n_col)

    def d_a(i, c):
        return to_col(pb.at[i, c], rcv_a.at[i, c], a_s.at[i, c], a_r.at[i, c], pair)

    def d_b(i, c):
        return to_col(pb.at[i, c], rcv_b.at[i, c], b_s.at[i, c], b_r.at[i, c], across)

    def d_u(i, k, c):
        return to_col(u.at[i, k, c], u.at[i, k, c], u_s.at[i, c], u_r.at[i, c], pair)

    def d_px(i, p, j):
        return to_scen(px.at[i, p, ms], px.at[i, p, ms], px_s.at[i, p, j - 1], px_r.at[i, p, j - 1], j)

    def d_c1(i, k, j):
        return to_col(sc1.at[i, k, mc], sc1.at[i, k, mc], c1_s.at[i, k, j - 1], c1_r.at[i, k, j - 1], col_peer(j))

    def d_c2(i, j):
        return to_scen(sc2.at[i, ms], sc2.at[i, ms], c2_s.at[i, j - 1], c2_r.at[i, j - 1], j)

    lane_no = lax.broadcasted_iota(jnp.int32, (8, 128), 1)
    lane_group = lane_no // W

    def pack(parts):
        out = jnp.zeros((8, 128), f32)
        for n, x in enumerate(parts):
            tot = jnp.broadcast_to(jnp.sum(x, axis=1, keepdims=True), (K, 128))
            for k in range(G):
                out = jnp.where(lane_group == n * G + k, tot[8 * k:8 * k + 8], out)
        return out

    def unpack(p):
        return [jnp.concatenate(
            [jnp.broadcast_to(
                jnp.sum(jnp.where(lane_no == W * (n * G + k), p, 0.0), axis=1, keepdims=True), (8, 128))
             for k in range(G)], axis=0) for n in range(5)]

    def lanes(x):
        out = x[:, 0:128]
        for k in range(1, x.shape[1] // 128):
            out = out + x[:, 128 * k:128 * k + 128]
        return out

    def rows_of(c):
        return c // H, pl.ds(pl.multiple_of(lax.rem(c, H) * RH, RH), RH)

    def load_t(c):
        s, rows = rows_of(c)
        return pltpu.make_async_copy(tech_hbm.at[s, rows, :], wts.at[c, :, pl.ds(0, C1)], ld_t.at[c])

    def load_r(c):
        s, rows = rows_of(c)
        return pltpu.make_async_copy(rec_hbm.at[s, rows, :], wts.at[c, :, pl.ds(C1, C2)], ld_r.at[c])

    def load_g(i, c):
        s, rows = rows_of(c)
        return pltpu.make_async_copy(rhs_hbm.at[s, pl.ds(i * K, K), rows], g.at[i, c], ld_g.at[i, c])

    def each(n, f):
        def one(c, carry):
            f(c)
            return carry
        lax.fori_loop(0, n, one, 0)

    def load_all(c):
        load_g(0, c).start()
        load_g(1, c).start()
        load_t(c).start()
        load_r(c).start()

    each(N, load_all)

    barrier = pltpu.get_barrier_semaphore()
    for j in SJ:
        pl.semaphore_signal(barrier, inc=1, device_id=(scen_peer(j), mc), device_id_type=pl.DeviceIdType.MESH)
    for j in CJ:
        pl.semaphore_signal(barrier, inc=1, device_id=(ms, col_peer(j)), device_id_type=pl.DeviceIdType.MESH)

    for ref in (bq1, dir1, sol1, bq2, dir2, sol2, uu, uv, uw, nres, dirn, qn, rat, dual, u, acc, bk2):
        ref[...] = jnp.zeros_like(ref)

    def init_cones(s):
        ids = cid[pl.ds(s, 1), :]
        onehot[s] = (lax.broadcasted_iota(jnp.int32, (NCONE, R), 0) == ids).astype(f32).astype(bf16)

    each(S, init_cones)

    def add_back(i, s, f):
        acc[i] = acc[i] + f[:, 0:C1]
        bk2[i, s] = bk2[i, s] + f[:, C1:C1 + C2]

    def back(i, c, z):
        add_back(i, c // H, jnp.dot(z, wts[c], preferred_element_type=f32))

    def first_back(c):
        load_g(0, c).wait()
        load_g(1, c).wait()
        load_t(c).wait()
        load_r(c).wait()
        z = jnp.concatenate([g[0, c], g[1, c]], axis=0).astype(bf16)
        f = jnp.dot(z, wts[c], preferred_element_type=f32)
        add_back(0, c // H, f[0:K])
        add_back(1, c // H, f[K:2 * K])
        for j in range((C1 + C2) // CB):
            cols = slice(j * CB, (j + 1) * CB)
            wtt[c, cols, :] = wts[c, :, cols].T

    each(N, first_back)
    pl.semaphore_wait(barrier, n_scen + n_col - 2)

    def send_first(i, p):
        px[i, p, ms] = acc[i].astype(bf16)
        for j in SJ:
            d_px(i, p, j).start()

    def take_first(i, p):
        for j in SJ:
            d_px(i, p, j).wait_recv()
        tot = px[i, p, 0].astype(f32)
        for k in range(1, n_scen):
            tot = tot + px[i, p, k].astype(f32)
        for j in SJ:
            d_px(i, p, j).wait_send()
        return tot

    def new_direction(i, k):
        r1 = res1[i]
        xin[i] = r1.astype(bf16)
        sq = lanes(r1 * r1) * (1.0 / n_scen)
        cr = lanes(r1 * dir1[i]) * (1.0 / n_scen)
        for s in range(S):
            r2 = res2[i, s]
            sq = sq + lanes(r2 * r2)
            cr = cr + lanes(r2 * dir2[i, s])
        sc1[i, k, mc] = pack([sq, cr])
        for j in CJ:
            d_c1(i, k, j).start()

    def restart(i):
        res1[i] = take_first(i, 1) - cost1[...]
        for s in range(S):
            res2[i, s] = bk2[i, s] - cost2[s:s + 1, :]
        new_direction(i, 0)

    send_first(0, 1)
    send_first(1, 1)
    restart(0)

    def front(i, c):
        x = jnp.concatenate([xin[i], res2[i, c // H].astype(bf16)], axis=1)
        return jnp.dot(x, wtt[c], preferred_element_type=f32)

    def relay(i, c):
        d_a(i, c).wait_recv()
        pb[i, c] = (part[c] + rcv_a[i, c].astype(f32)).astype(bf16)
        d_b(i, c).start()

    def finish_rows(i, k, c):
        @pl.when(is_end)
        def _():
            d_u(i, k, c).wait_recv()

        @pl.when(is_mid)
        def _():
            d_b(i, c).wait_recv()
            u[i, k, c] = (pb[i, c].astype(f32) + rcv_b[i, c].astype(f32)).astype(bf16)
            d_u(i, k, c).start()

        v = u[i, k, c].astype(f32)
        before = u[i, lax.rem(k + CG_STEPS - 1, CG_STEPS), c].astype(f32)
        earlier = u[i, lax.rem(k + CG_STEPS - 2, CG_STEPS), c].astype(f32)
        uu[i] = uu[i] + lanes(v * v)
        uv[i] = uv[i] + lanes(v * before)
        uw[i] = uw[i] + lanes(v * earlier)

    def send_scalars(i, k):
        total = pack([jnp.zeros((K, 128), f32)] * 2 + [uu[i], uv[i], uw[i]])
        for j in CJ:
            d_c1(i, k, j).wait_recv()
        for m in range(n_col):
            total = total + sc1[i, k, m]
        for j in CJ:
            d_c1(i, k, j).wait_send()
        sc2[i, ms] = total
        for j in SJ:
            d_c2(i, j).start()

    def finish_scalars(i, k):
        for j in SJ:
            d_c2(i, j).wait_recv()
        total = sc2[i, 0]
        for m in range(1, n_scen):
            total = total + sc2[i, m]
        for j in SJ:
            d_c2(i, j).wait_send()
        s0, s1, s2, s3, s4 = unpack(total)
        r = jnp.where(k == 0, 0.0, s0 / nres[i])
        dn = s0 + r * (2.0 * s1 + r * dirn[i])
        qs = s2 + r * (2.0 * (s3 + rat[i] * s4) + r * qn[i])
        nres[i] = s0
        dirn[i] = dn
        qn[i] = qs
        rat[i] = r
        rats[i, k] = r
        a = s0 / (dn + qs)
        alphas[i, k] = a
        r, a = r[:, 0:1], a[:, 0:1]
        d1 = res1[i] + r * dir1[i]
        dir1[i] = d1
        sol1[i] = sol1[i] + a * d1
        for s in range(S):
            d2 = res2[i, s] + r * dir2[i, s]
            dir2[i, s] = d2
            sol2[i, s] = sol2[i, s] + a * d2

    def next_residual(i, k):
        r, a = rats[i, k][:, 0:1], alphas[i, k][:, 0:1]
        q1 = take_first(i, lax.rem(k, 2)) + r * bq1[i]
        bq1[i] = q1
        res1[i] = res1[i] - a * (dir1[i] + q1)
        for s in range(S):
            q2 = bk2[i, s] + r * bq2[i, s]
            bq2[i, s] = q2
            res2[i, s] = res2[i, s] - a * (dir2[i, s] + q2)
        new_direction(i, k + 1)

    def all_sent(i, k):
        @pl.when(is_end)
        def _():
            each(N, lambda c: d_a(i, c).wait_send())

        @pl.when(is_mid)
        def _():
            def one(c):
                d_b(i, c).wait_send()
                d_u(i, k, c).wait_send()

            each(N, one)

    def split(x):
        hi = x.astype(bf16)
        return [hi, (x - hi.astype(f32)).astype(bf16)]

    def project(i):
        c2 = alphas[i, 2]
        c1 = alphas[i, 1] + rats[i, 2] * c2
        c0 = alphas[i, 0] + rats[i, 1] * c1
        c0, c1, c2 = c0[:, 0:1], c1[:, 0:1], c2[:, 0:1]

        def one(s):
            st = starts[pl.ds(s, 1), :]
            pieces = []
            for h in range(H):
                c = s * H + h
                piece = g[i, c] - (c0 * u[i, 0, c].astype(f32) + c1 * u[i, 1, c].astype(f32)
                                   + c2 * u[i, 2, c].astype(f32))
                g[i, c] = piece
                pieces.append(piece)
            gs = jnp.concatenate(pieces, axis=1)
            v = gs - jnp.concatenate([dual[i, s * H + h] for h in range(H)], axis=1)
            lead_v = v * st
            tail_v = v * v * (1.0 - st)
            stack = jnp.concatenate(split(lead_v) + split(tail_v), axis=0)
            sums = lax.dot_general(stack, onehot[s], (((1,), (1,)), ((), ())), preferred_element_type=f32)
            lead = sums[0:K] + sums[K:2 * K]
            tail = sums[2 * K:3 * K] + sums[3 * K:4 * K]
            head, scale = cone_factors(lead, tail)
            stack2 = jnp.concatenate(split(head) + split(scale), axis=0)
            outs = jnp.dot(stack2, onehot[s], preferred_element_type=f32)
            head_rows = outs[0:K] + outs[K:2 * K]
            scale_rows = outs[2 * K:3 * K] + outs[3 * K:4 * K]
            sl = st * head_rows + (1.0 - st) * v * scale_rows
            du = sl - v
            d = (gs - sl - du).astype(bf16)
            for h in range(H):
                cols = slice(h * RH, (h + 1) * RH)
                slack[i, s * H + h] = sl[:, cols]
                dual[i, s * H + h] = du[:, cols]
                dz[s * H + h] = d[:, cols]

        each(S, one)

    def turn(t, carry):
        a = lax.rem(t, 2)
        b = 1 - a
        ka = lax.rem(t // 2, CG_STEPS + 1)
        kb = lax.rem((t + 2 * CG_STEPS + 1) // 2, CG_STEPS + 1)
        run_a, run_b = ka < CG_STEPS, kb < CG_STEPS
        back_a, back_b = ka < CG_STEPS - 1, kb < CG_STEPS - 1
        acc[a] = jnp.zeros((K, C1), f32)
        bk2[a] = jnp.zeros((S, K, C2), f32)
        uu[a] = jnp.zeros((K, 128), f32)
        uv[a] = jnp.zeros((K, 128), f32)
        uw[a] = jnp.zeros((K, 128), f32)

        def slot(k):
            @pl.when(jnp.logical_and(run_a, k < N))
            def _():
                p = front(a, k)

                @pl.when(is_end)
                def _():
                    pb[a, k] = p.astype(bf16)
                    d_a(a, k).start()

                @pl.when(is_mid)
                def _():
                    part[k] = p

            @pl.when(jnp.logical_and(run_b, k < TAIL))
            def _():
                c = N - TAIL + k
                finish_rows(b, kb, c)

                @pl.when(back_b)
                def _():
                    back(b, c, u[b, kb, c])

                @pl.when(k == TAIL - 1)
                def _():
                    @pl.when(back_b)
                    def _():
                        send_first(b, lax.rem(kb, 2))

                    send_scalars(b, kb)

            @pl.when(jnp.logical_and(jnp.logical_and(run_a, is_mid), k >= LAG_A))
            def _():
                relay(a, k - LAG_A)

            @pl.when(jnp.logical_and(run_a, jnp.logical_and(k >= lag, k < lag + N - TAIL)))
            def _():
                c = k - lag
                finish_rows(a, ka, c)

                @pl.when(back_a)
                def _():
                    back(a, c, u[a, ka, c])

        each(SLOTS, slot)

        @pl.when(ka == CG_STEPS)
        def _():
            project(a)

            @pl.when(t < TURNS - 2)
            def _():
                each(N, lambda c: back(a, c, dz[c]))
                send_first(a, 1)

        @pl.when(run_b)
        def _():
            finish_scalars(b, kb)
            all_sent(b, kb)

        @pl.when(back_b)
        def _():
            next_residual(b, kb)

        @pl.when(jnp.logical_and(kb == CG_STEPS, t < TURNS - 1))
        def _():
            restart(b)

        return carry

    lax.fori_loop(0, TURNS, turn, 0)

    RQ = R // n_col
    own = mc * RQ // RH
    here = pl.ds(pl.multiple_of(lax.rem(mc * RQ, RH), 128), RQ)
    for i in range(2):
        rows = slice(i * K, (i + 1) * K)
        x_out[rows, :] = sol1[i]
        for s in range(S):
            y_out[s, rows, :] = sol2[i, s]
            slack_out[s, rows, :] = slack[i, s * H + own, :, here]
            dual_out[s, rows, :] = dual[i, s * H + own, :, here]


def fused(tech, recourse, rhs, cost_first, cost_second, cone_id):
    f32, bf16 = jnp.float32, jnp.bfloat16
    n_scen = lax.axis_size("scen")
    n_col = lax.axis_size("col")
    B = rhs.shape[0]
    S, R, C1 = tech.shape
    C2 = recourse.shape[2]
    RQ = R // n_col
    RH = R // CHUNKS
    N = S * CHUNKS
    K = B // 2
    starts = jnp.concatenate(
        [jnp.ones((S, 1), f32), (cone_id[:, 1:] != cone_id[:, :-1]).astype(f32)], axis=1)
    vm = pl.BlockSpec(memory_space=pltpu.VMEM)
    hbm = pl.BlockSpec(memory_space=pl.ANY)
    V = pltpu.VMEM
    D = pltpu.SemaphoreType.DMA
    ns, nc = n_scen - 1, n_col - 1
    rows = lambda dt: V((2, N, K, RH), dt)
    one = V((2, K, C1), f32)
    two = V((2, S, K, C2), f32)
    num = V((2, K, 128), f32)
    scratch = [
        V((N, RH, C1 + C2), bf16), V((N, C1 + C2, RH), bf16),
        rows(f32), rows(f32), rows(f32), V((S, NCONE, R), bf16), V((N, K, RH), f32),
        rows(bf16), rows(bf16), rows(bf16), V((2, CG_STEPS, N, K, RH), bf16), V((N, K, RH), bf16),
        V((2, 2, n_scen, K, C1), bf16), one, one, one, one, one, V((2, K, C1), bf16),
        two, two, two, two, two,
        V((2, CG_STEPS, n_col, 8, 128), f32), V((2, n_scen, 8, 128), f32), num, num, num,
        num, num, num, num, V((2, CG_STEPS, K, 128), f32), V((2, CG_STEPS, K, 128), f32),
        D((N,)), D((N,)), D((2, N)),
        D((2, N)), D((2, N)), D((2, N)), D((2, N)), D((2, N)), D((2, N)),
        D((2, 2, ns)), D((2, 2, ns)), D((2, CG_STEPS, nc)), D((2, CG_STEPS, nc)), D((2, ns)), D((2, ns)),
    ]
    x, y, slack, dual = pl.pallas_call(
        functools.partial(kernel_body, (n_scen, n_col, B, S, R, C1, C2)),
        out_shape=(
            jax.ShapeDtypeStruct((B, C1), f32),
            jax.ShapeDtypeStruct((S, B, C2), f32),
            jax.ShapeDtypeStruct((S, B, RQ), f32),
            jax.ShapeDtypeStruct((S, B, RQ), f32),
        ),
        in_specs=[hbm, hbm, hbm, vm, vm, vm, vm],
        out_specs=(vm, vm, vm, vm),
        scratch_shapes=scratch,
        compiler_params=pltpu.CompilerParams(
            collective_id=0, has_side_effects=True, vmem_limit_bytes=62 * 1024 * 1024),
    )(
        tech, recourse, jnp.transpose(rhs, (1, 0, 2)),
        cost_first.reshape(1, C1), cost_second, cone_id, starts,
    )
    back = lambda a: jnp.transpose(a, (1, 0, 2))
    return x, back(y), back(slack), back(dual)


def program(tech, recourse, rhs, cost_first, cost_second, cone_id):
    n_scen = lax.axis_size("scen")
    n_col = lax.axis_size("col")
    batch = rhs.shape[0]
    fits = (
        (tech.shape[2] + recourse.shape[2]) % 256 == 0
        and tech.shape[2] % (128 * n_scen) == 0
        and tech.shape[1] % (128 * n_col) == 0
        and recourse.shape[2] % 128 == 0
        and batch % 32 == 0
        and batch <= 256
        and n_scen > 1
        and n_col == 4
    )
    run = fused if fits else body
    return run(tech, recourse, rhs, cost_first, cost_second, cone_id)


def solution(mesh):
    placed = (
        P("scen", None, "col"),
        P("scen", None, "col"),
        P(None, "scen", None),
        P("col"),
        P("scen", "col"),
        P("scen", None),
    )
    return jax.shard_map(
        program,
        mesh=mesh,
        in_specs=placed,
        out_specs=(
            P(None, "col"),
            P(None, "scen", "col"),
            P(None, "scen", "col"),
            P(None, "scen", "col"),
        ),
        check_vma=False,
    )
```

```python
import functools

import jax
import jax.numpy as jnp
from jax import lax
from jax.experimental import pallas as pl
from jax.experimental.pallas import tpu as pltpu
from jax.sharding import PartitionSpec as P

NCONE = 128
ITERS = 3
CG_STEPS = 3
CHUNKS = 2
LAG_A = 4
LAG_B = 7
LAG_E = 7
TAIL_M = 3
TAIL_E = 6
FROM_M = 0
FROM_E = 0


HIGH = lax.Precision.HIGHEST


def cone_factors(lead, tail):
    norm_tail = jnp.sqrt(tail)
    inside = norm_tail <= lead
    polar = norm_tail <= -lead
    safe = jnp.where(norm_tail > 0.0, norm_tail, 1.0)
    middle = 0.5 * (lead + norm_tail)
    head = jnp.where(inside, lead, jnp.where(polar, 0.0, middle))
    scale = jnp.where(inside, 1.0, jnp.where(polar, 0.0, middle / safe))
    return (head, scale)


def body(tech, recourse, rhs, cost_first, cost_second, cone_id):
    f32 = jnp.float32
    bf16 = jnp.bfloat16
    n_scen = lax.axis_size("scen")
    n_col = lax.axis_size("col")
    batch = rhs.shape[0]
    scen_local = tech.shape[0]
    rows = tech.shape[1]
    first_cols = tech.shape[2]
    tech_flat = tech.reshape(scen_local * rows, first_cols)
    starts = jnp.concatenate(
        [jnp.ones((scen_local, 1), f32), (cone_id[:, 1:] != cone_id[:, :-1]).astype(f32)], axis=1
    )
    labels = lax.broadcasted_iota(jnp.int32, (1, 1, NCONE), 2)
    onehot = (cone_id[:, :, None] == labels).astype(f32)
    part_rows = rows // n_col
    row_start = lax.axis_index("col") * part_rows
    row_weight = 1.0 / n_col
    share_cols = first_cols // n_scen
    cost_here = lax.dynamic_slice_in_dim(
        cost_first, lax.axis_index("scen") * share_cols, share_cols, 0
    )
    first_weight = 1.0
    start_rows = starts[None]

    def couple(partial_value):
        return lax.psum_scatter(partial_value, "scen", scatter_dimension=1, tiled=True)

    def adjoint(rows_bf):
        first_part = jnp.dot(
            rows_bf.reshape(batch, scen_local * rows), tech_flat, preferred_element_type=f32
        )
        second_part = jnp.einsum("bsm,smk->bsk", rows_bf, recourse, preferred_element_type=f32)
        return (first_part, second_part)

    def local_squares(first_vec, second_vec):
        return first_weight * jnp.sum(first_vec * first_vec, axis=1) + jnp.sum(
            second_vec * second_vec, axis=(1, 2)
        )

    def total_norm(first_vec, second_vec):
        return lax.psum(local_squares(first_vec, second_vec), ("scen", "col"))

    here_rows = rhs.shape[2]
    first_sol = jnp.zeros((batch, share_cols), f32)
    second_sol = jnp.zeros((batch, scen_local, recourse.shape[2]), f32)
    slack = jnp.zeros((batch, scen_local, here_rows), f32)
    dual = jnp.zeros((batch, scen_local, here_rows), f32)
    image = jnp.zeros((batch, scen_local, here_rows), f32)
    for outer in range(ITERS):
        resid_rows = (rhs - slack - dual - image).astype(bf16)
        back_first, back_second = adjoint(resid_rows)
        res_first = couple(back_first) - cost_here[None, :]
        res_second = back_second - cost_second[None]
        res_norm = total_norm(res_first, res_second)
        dir_first, dir_second = (res_first, res_second)
        for step in range(CG_STEPS):
            dir_first_bf = lax.all_gather(dir_first.astype(bf16), "scen", axis=1, tiled=True)
            forward_partial_value = lax.dot_general(
                dir_first_bf, tech_flat, (((1,), (1,)), ((), ())), preferred_element_type=f32
            )
            forward_partial_value = forward_partial_value.reshape(batch, scen_local, rows)
            image_step = lax.psum(
                forward_partial_value
                + jnp.einsum(
                    "bsk,smk->bsm", dir_second.astype(bf16), recourse, preferred_element_type=f32
                ),
                "col",
            )
            curv_term = local_squares(dir_first, dir_second) + row_weight * jnp.sum(
                image_step * image_step, axis=(1, 2)
            )
            curv = lax.psum(curv_term, ("scen", "col"))
            alpha = res_norm / curv
            first_sol = first_sol + alpha[:, None] * dir_first
            second_sol = second_sol + alpha[:, None, None] * dir_second
            image = image + alpha[:, None, None] * image_step
            if step + 1 < CG_STEPS:
                back_first, back_second = adjoint(image_step.astype(bf16))
                res_first = res_first - alpha[:, None] * (dir_first + couple(back_first))
                res_second = res_second - alpha[:, None, None] * (dir_second + back_second)
                new_norm = total_norm(res_first, res_second)
                ratio = new_norm / res_norm
                dir_first = res_first + ratio[:, None] * dir_first
                dir_second = res_second + ratio[:, None, None] * dir_second
                res_norm = new_norm
        values = rhs - image - dual
        project_lead = jnp.einsum("bsm,smc->bsc", values * start_rows, onehot, precision=HIGH)
        project_tail = jnp.einsum(
            "bsm,smc->bsc", values * values * (1.0 - start_rows), onehot, precision=HIGH
        )
        project_lead, project_tail = (project_lead, project_tail)
        head, scale = cone_factors(project_lead, project_tail)
        head_rows = jnp.einsum("bsc,smc->bsm", head, onehot, precision=HIGH)
        scale_rows = jnp.einsum("bsc,smc->bsm", scale, onehot, precision=HIGH)
        slack = start_rows * head_rows + (1.0 - start_rows) * values * scale_rows
        dual = dual + image + slack - rhs
    first_out = lax.all_gather(first_sol, "scen", axis=1, tiled=True)
    slack_out = lax.dynamic_slice_in_dim(slack, row_start, part_rows, 2)
    dual_out = lax.dynamic_slice_in_dim(dual, row_start, part_rows, 2)
    return (first_out, second_sol, slack_out, dual_out)


def kernel_body(
    dims,
    tech_hbm, rec_hbm, rhs_hbm, cost1, cost2, cid,
    x_out, y_out, slack_out, dual_out,
    wts, wtt, g, dual, slack, onehot, part, pb, rcv_a, rcv_b, u, dz,
    px, acc, bq1, res1, dir1, sol1, xin, bk2, bq2, res2, dir2, sol2,
    sc1, sc2, uu, uv, uw,
    nres, dirn, qn, rat, alphas, rats,
    ld_t, ld_r, ld_g,
    a_s, a_r, b_s, b_r, u_s, u_r, px_s, px_r, c1_s, c1_r, c2_s, c2_r,
):
    n_scen, n_col, B, S, R, C1, C2 = dims
    f32, bf16 = jnp.float32, jnp.bfloat16
    H = CHUNKS
    RH = R // H
    N = S * H
    K = B // 2
    CB = 256
    G = K // 8
    W = 128 // (5 * G)
    SLOTS = max(N + LAG_A, LAG_B + N - TAIL_M, LAG_E + N - TAIL_E)
    TURNS = 2 * ITERS * (CG_STEPS + 1)
    ms = lax.axis_index("scen")
    mc = lax.axis_index("col")
    pair = mc + 1 - 2 * lax.rem(mc, 2)
    across = 3 - mc
    is_end = jnp.logical_or(mc == 0, mc == 3)
    is_mid = jnp.logical_or(mc == 1, mc == 2)
    mid = lax.rem((mc + 1) // 2, 2)
    lag = LAG_E + (LAG_B - LAG_E) * mid
    tail = TAIL_E + (TAIL_M - TAIL_E) * mid
    tail_from = FROM_E + (FROM_M - FROM_E) * mid
    project_from = TAIL_M * mid

    def scen_peer(j):
        out = 0
        for bit in range(n_scen.bit_length() - 1):
            own = lax.rem(ms // (1 << bit), 2)
            out = out + (1 << bit) * (1 - own if j >> bit & 1 else own)
        return out

    def col_peer(j):
        return lax.rem(mc + j, n_col)

    def to_scen(src, dst, ss, rs, j):
        return pltpu.make_async_remote_copy(
            src_ref=src, dst_ref=dst, send_sem=ss, recv_sem=rs,
            device_id=(scen_peer(j), mc), device_id_type=pl.DeviceIdType.MESH)

    def to_col(src, dst, ss, rs, target):
        return pltpu.make_async_remote_copy(
            src_ref=src, dst_ref=dst, send_sem=ss, recv_sem=rs,
            device_id=(ms, target), device_id_type=pl.DeviceIdType.MESH)

    SJ = sorted(range(1, n_scen), key=lambda j: -bin(j >> 1).count("1"))
    CJ = range(1, n_col)

    def d_a(i, c):
        return to_col(pb.at[i, c], rcv_a.at[i, c], a_s.at[i, c], a_r.at[i, c], pair)

    def d_b(i, c):
        return to_col(pb.at[i, c], rcv_b.at[i, c], b_s.at[i, c], b_r.at[i, c], across)

    def d_u(i, k, c):
        return to_col(u.at[i, k, c], u.at[i, k, c], u_s.at[i, c], u_r.at[i, c], pair)

    def d_px(i, p, j):
        return to_scen(px.at[i, p, ms], px.at[i, p, ms], px_s.at[i, p, j - 1], px_r.at[i, p, j - 1], j)

    def d_c1(i, k, j):
        return to_col(sc1.at[i, k, mc], sc1.at[i, k, mc], c1_s.at[i, k, j - 1], c1_r.at[i, k, j - 1], col_peer(j))

    def d_c2(i, j):
        return to_scen(sc2.at[i, ms], sc2.at[i, ms], c2_s.at[i, j - 1], c2_r.at[i, j - 1], j)

    lane_no = lax.broadcasted_iota(jnp.int32, (8, 128), 1)
    lane_group = lane_no // W

    def pack(parts):
        out = jnp.zeros((8, 128), f32)
        for n, x in enumerate(parts):
            tot = jnp.broadcast_to(jnp.sum(x, axis=1, keepdims=True), (K, 128))
            for k in range(G):
                out = jnp.where(lane_group == n * G + k, tot[8 * k:8 * k + 8], out)
        return out

    def unpack(p):
        return [jnp.concatenate(
            [jnp.broadcast_to(
                jnp.sum(jnp.where(lane_no == W * (n * G + k), p, 0.0), axis=1, keepdims=True), (8, 128))
             for k in range(G)], axis=0) for n in range(5)]

    def lanes(x):
        out = x[:, 0:128]
        for k in range(1, x.shape[1] // 128):
            out = out + x[:, 128 * k:128 * k + 128]
        return out

    def rows_of(c):
        return c // H, pl.ds(pl.multiple_of(lax.rem(c, H) * RH, RH), RH)

    def load_t(c):
        s, rows = rows_of(c)
        return pltpu.make_async_copy(tech_hbm.at[s, rows, :], wts.at[c, :, pl.ds(0, C1)], ld_t.at[c])

    def load_r(c):
        s, rows = rows_of(c)
        return pltpu.make_async_copy(rec_hbm.at[s, rows, :], wts.at[c, :, pl.ds(C1, C2)], ld_r.at[c])

    def load_g(i, c):
        s, rows = rows_of(c)
        return pltpu.make_async_copy(rhs_hbm.at[pl.ds(i * K, K), s, rows], g.at[i, c], ld_g.at[i, c])

    def each(n, f):
        def one(c, carry):
            f(c)
            return carry
        lax.fori_loop(0, n, one, 0)

    def load_all(c):
        load_g(0, c).start()
        load_g(1, c).start()
        load_t(c).start()
        load_r(c).start()

    each(N, load_all)

    barrier = pltpu.get_barrier_semaphore()
    for j in SJ:
        pl.semaphore_signal(barrier, inc=1, device_id=(scen_peer(j), mc), device_id_type=pl.DeviceIdType.MESH)
    for j in CJ:
        pl.semaphore_signal(barrier, inc=1, device_id=(ms, col_peer(j)), device_id_type=pl.DeviceIdType.MESH)

    for ref in (bq1, dir1, sol1, bq2, dir2, sol2, uu, uv, uw, nres, dirn, qn, rat, dual, u, acc, bk2):
        ref[...] = jnp.zeros_like(ref)

    def init_cones(s):
        ids = cid[pl.ds(s, 1), :]
        onehot[s] = (lax.broadcasted_iota(jnp.int32, (NCONE, R), 0) == ids).astype(f32).astype(bf16)

    each(S, init_cones)

    def add_back(i, s, f):
        acc[i] = acc[i] + f[:, 0:C1]
        bk2[i, s] = bk2[i, s] + f[:, C1:C1 + C2]

    def back(i, c, z):
        add_back(i, c // H, jnp.dot(z, wts[c], preferred_element_type=f32))

    def first_back(c):
        load_g(0, c).wait()
        load_g(1, c).wait()
        load_t(c).wait()
        load_r(c).wait()
        z = jnp.concatenate([g[0, c], g[1, c]], axis=0).astype(bf16)
        f = jnp.dot(z, wts[c], preferred_element_type=f32)
        add_back(0, c // H, f[0:K])
        add_back(1, c // H, f[K:2 * K])
        for j in range((C1 + C2) // CB):
            cols = slice(j * CB, (j + 1) * CB)
            wtt[c, cols, :] = wts[c, :, cols].T

    each(N, first_back)
    pl.semaphore_wait(barrier, n_scen + n_col - 2)

    def send_first(i, p):
        px[i, p, ms] = acc[i].astype(bf16)
        for j in SJ:
            d_px(i, p, j).start()

    def take_first(i, p):
        for j in SJ:
            d_px(i, p, j).wait_recv()
        tot = px[i, p, 0].astype(f32)
        for k in range(1, n_scen):
            tot = tot + px[i, p, k].astype(f32)
        for j in SJ:
            d_px(i, p, j).wait_send()
        return tot

    def send_norms(i, k):
        r1 = res1[i]
        sq = lanes(r1 * r1) * (1.0 / n_scen)
        cr = lanes(r1 * dir1[i]) * (1.0 / n_scen)
        for s in range(S):
            r2 = res2[i, s]
            sq = sq + lanes(r2 * r2)
            cr = cr + lanes(r2 * dir2[i, s])
        sc1[i, k, mc] = pack([sq, cr])
        for j in CJ:
            d_c1(i, k, j).start()

    def restart(i):
        r1 = take_first(i, 1) - cost1[...]
        res1[i] = r1
        xin[i] = r1.astype(bf16)
        for s in range(S):
            res2[i, s] = bk2[i, s] - cost2[s:s + 1, :]

    send_first(0, 1)
    send_first(1, 1)
    restart(0)

    def front(i, c):
        x = jnp.concatenate([xin[i], res2[i, c // H].astype(bf16)], axis=1)
        return jnp.dot(x, wtt[c], preferred_element_type=f32)

    def relay(i, c):
        d_a(i, c).wait_recv()
        pb[i, c] = (part[c] + rcv_a[i, c].astype(f32)).astype(bf16)
        d_b(i, c).start()

    def finish_rows(i, k, c):
        @pl.when(is_end)
        def _():
            d_u(i, k, c).wait_recv()

        @pl.when(is_mid)
        def _():
            d_b(i, c).wait_recv()
            u[i, k, c] = (pb[i, c].astype(f32) + rcv_b[i, c].astype(f32)).astype(bf16)
            d_u(i, k, c).start()

        v = u[i, k, c].astype(f32)
        before = u[i, lax.rem(k + CG_STEPS - 1, CG_STEPS), c].astype(f32)
        earlier = u[i, lax.rem(k + CG_STEPS - 2, CG_STEPS), c].astype(f32)
        uu[i] = uu[i] + lanes(v * v)
        uv[i] = uv[i] + lanes(v * before)
        uw[i] = uw[i] + lanes(v * earlier)

    def send_scalars(i, k):
        total = pack([jnp.zeros((K, 128), f32)] * 2 + [uu[i], uv[i], uw[i]])
        for j in CJ:
            d_c1(i, k, j).wait_recv()
        for m in range(n_col):
            total = total + sc1[i, k, m]
        for j in CJ:
            d_c1(i, k, j).wait_send()
        sc2[i, ms] = total
        for j in SJ:
            d_c2(i, j).start()

    def finish_scalars(i, k):
        for j in SJ:
            d_c2(i, j).wait_recv()
        total = sc2[i, 0]
        for m in range(1, n_scen):
            total = total + sc2[i, m]
        for j in SJ:
            d_c2(i, j).wait_send()
        s0, s1, s2, s3, s4 = unpack(total)
        r = jnp.where(k == 0, 0.0, s0 / nres[i])
        dn = s0 + r * (2.0 * s1 + r * dirn[i])
        qs = s2 + r * (2.0 * (s3 + rat[i] * s4) + r * qn[i])
        nres[i] = s0
        dirn[i] = dn
        qn[i] = qs
        rat[i] = r
        rats[i, k] = r
        a = s0 / (dn + qs)
        alphas[i, k] = a
        r, a = r[:, 0:1], a[:, 0:1]
        d1 = res1[i] + r * dir1[i]
        dir1[i] = d1
        sol1[i] = sol1[i] + a * d1
        for s in range(S):
            d2 = res2[i, s] + r * dir2[i, s]
            dir2[i, s] = d2
            sol2[i, s] = sol2[i, s] + a * d2

    def next_residual(i, k):
        r, a = rats[i, k][:, 0:1], alphas[i, k][:, 0:1]
        q1 = take_first(i, lax.rem(k, 2)) + r * bq1[i]
        bq1[i] = q1
        r1 = res1[i] - a * (dir1[i] + q1)
        res1[i] = r1
        xin[i] = r1.astype(bf16)
        for s in range(S):
            q2 = bk2[i, s] + r * bq2[i, s]
            bq2[i, s] = q2
            res2[i, s] = res2[i, s] - a * (dir2[i, s] + q2)

    def all_sent(i, k):
        @pl.when(is_end)
        def _():
            each(N, lambda c: d_a(i, c).wait_send())

        @pl.when(is_mid)
        def _():
            def one(c):
                d_b(i, c).wait_send()
                d_u(i, k, c).wait_send()

            each(N, one)

    def split(x):
        hi = x.astype(bf16)
        return [hi, (x - hi.astype(f32)).astype(bf16)]

    def project(i, s):
        c2 = alphas[i, 2]
        c1 = alphas[i, 1] + rats[i, 2] * c2
        c0 = alphas[i, 0] + rats[i, 1] * c1
        c0, c1, c2 = c0[:, 0:1], c1[:, 0:1], c2[:, 0:1]
        ids = cid[pl.ds(s, 1), :]
        first = lax.broadcasted_iota(jnp.int32, (1, R), 1) == 0
        st = jnp.where(jnp.logical_or(first, ids != pltpu.roll(ids, 1, 1)), 1.0, 0.0)
        pieces = []
        for h in range(H):
            c = s * H + h
            piece = g[i, c] - (c0 * u[i, 0, c].astype(f32) + c1 * u[i, 1, c].astype(f32)
                               + c2 * u[i, 2, c].astype(f32))
            g[i, c] = piece
            pieces.append(piece)
        gs = jnp.concatenate(pieces, axis=1)
        v = gs - jnp.concatenate([dual[i, s * H + h] for h in range(H)], axis=1)
        lead_v = v * st
        tail_v = v * v * (1.0 - st)
        stack = jnp.concatenate(split(lead_v) + split(tail_v), axis=0)
        sums = lax.dot_general(stack, onehot[s], (((1,), (1,)), ((), ())), preferred_element_type=f32)
        lead = sums[0:K] + sums[K:2 * K]
        tail = sums[2 * K:3 * K] + sums[3 * K:4 * K]
        head, scale = cone_factors(lead, tail)
        stack2 = jnp.concatenate(split(head) + split(scale), axis=0)
        outs = jnp.dot(stack2, onehot[s], preferred_element_type=f32)
        head_rows = outs[0:K] + outs[K:2 * K]
        scale_rows = outs[2 * K:3 * K] + outs[3 * K:4 * K]
        sl = st * head_rows + (1.0 - st) * v * scale_rows
        du = sl - v
        d = (gs - sl - du).astype(bf16)
        for h in range(H):
            cols = slice(h * RH, (h + 1) * RH)
            slack[i, s * H + h] = sl[:, cols]
            dual[i, s * H + h] = du[:, cols]
            dz[s * H + h] = d[:, cols]

    def turn(t, carry):
        a = lax.rem(t, 2)
        b = 1 - a
        ka = lax.rem(t // 2, CG_STEPS + 1)
        kb = lax.rem((t + 2 * CG_STEPS + 1) // 2, CG_STEPS + 1)
        run_a, run_b = ka < CG_STEPS, kb < CG_STEPS
        back_a, back_b = ka < CG_STEPS - 1, kb < CG_STEPS - 1
        acc[a] = jnp.zeros((K, C1), f32)
        bk2[a] = jnp.zeros((S, K, C2), f32)
        uu[a] = jnp.zeros((K, 128), f32)
        uv[a] = jnp.zeros((K, 128), f32)
        uw[a] = jnp.zeros((K, 128), f32)

        def slot(k):
            @pl.when(jnp.logical_and(run_a, k < N))
            def _():
                p = front(a, k)

                @pl.when(is_end)
                def _():
                    pb[a, k] = p.astype(bf16)
                    d_a(a, k).start()

                @pl.when(is_mid)
                def _():
                    part[k] = p

            @pl.when(jnp.logical_and(run_a, k == 1))
            def _():
                send_norms(a, ka)

            @pl.when(jnp.logical_and(jnp.logical_not(run_a), jnp.logical_and(k >= project_from, k < project_from + S)))
            def _():
                project(a, k - project_from)

            @pl.when(jnp.logical_and(run_b, jnp.logical_and(k >= tail_from, k < tail_from + tail)))
            def _():
                c = N - tail + k - tail_from
                finish_rows(b, kb, c)

                @pl.when(k == tail_from + tail - 1)
                def _():
                    send_scalars(b, kb)

                @pl.when(back_b)
                def _():
                    back(b, c, u[b, kb, c])

                    @pl.when(k == tail_from + tail - 1)
                    def _():
                        send_first(b, lax.rem(kb, 2))

            @pl.when(jnp.logical_and(jnp.logical_and(run_a, is_mid), jnp.logical_and(k >= LAG_A, k < LAG_A + N)))
            def _():
                relay(a, k - LAG_A)

            @pl.when(jnp.logical_and(run_a, jnp.logical_and(k >= lag, k < lag + N - tail)))
            def _():
                c = k - lag
                finish_rows(a, ka, c)

                @pl.when(back_a)
                def _():
                    back(a, c, u[a, ka, c])

        each(SLOTS, slot)

        @pl.when(ka == CG_STEPS)
        def _():
            @pl.when(t < TURNS - 2)
            def _():
                each(N, lambda c: back(a, c, dz[c]))
                send_first(a, 1)

        @pl.when(run_b)
        def _():
            finish_scalars(b, kb)
            all_sent(b, kb)

        @pl.when(back_b)
        def _():
            next_residual(b, kb)

        @pl.when(jnp.logical_and(kb == CG_STEPS, t < TURNS - 1))
        def _():
            restart(b)

        return carry

    lax.fori_loop(0, TURNS, turn, 0)

    RQ = R // n_col
    own = mc * RQ // RH
    here = pl.ds(pl.multiple_of(lax.rem(mc * RQ, RH), 128), RQ)
    for i in range(2):
        rows = slice(i * K, (i + 1) * K)
        x_out[rows, :] = sol1[i]
        for s in range(S):
            y_out[s, rows, :] = sol2[i, s]
            slack_out[s, rows, :] = slack[i, s * H + own, :, here]
            dual_out[s, rows, :] = dual[i, s * H + own, :, here]


def lay_out(x, y, slack, dual, x_out, y_out, slack_out, dual_out):
    x_out[...] = x[...]
    for s in range(y.shape[0]):
        y_out[:, s, :] = y[s]
        slack_out[:, s, :] = slack[s]
        dual_out[:, s, :] = dual[s]


def fused(tech, recourse, rhs, cost_first, cost_second, cone_id):
    f32, bf16 = jnp.float32, jnp.bfloat16
    n_scen = lax.axis_size("scen")
    n_col = lax.axis_size("col")
    B = rhs.shape[0]
    S, R, C1 = tech.shape
    C2 = recourse.shape[2]
    RQ = R // n_col
    RH = R // CHUNKS
    N = S * CHUNKS
    K = B // 2
    vm = pl.BlockSpec(memory_space=pltpu.VMEM)
    hbm = pl.BlockSpec(memory_space=pl.ANY)
    V = pltpu.VMEM
    D = pltpu.SemaphoreType.DMA
    ns, nc = n_scen - 1, n_col - 1
    rows = lambda dt: V((2, N, K, RH), dt)
    one = V((2, K, C1), f32)
    two = V((2, S, K, C2), f32)
    num = V((2, K, 128), f32)
    scratch = [
        V((N, RH, C1 + C2), bf16), V((N, C1 + C2, RH), bf16),
        rows(f32), rows(f32), rows(f32), V((S, NCONE, R), bf16), V((N, K, RH), f32),
        rows(bf16), rows(bf16), rows(bf16), V((2, CG_STEPS, N, K, RH), bf16), V((N, K, RH), bf16),
        V((2, 2, n_scen, K, C1), bf16), one, one, one, one, one, V((2, K, C1), bf16),
        two, two, two, two, two,
        V((2, CG_STEPS, n_col, 8, 128), f32), V((2, n_scen, 8, 128), f32), num, num, num,
        num, num, num, num, V((2, CG_STEPS, K, 128), f32), V((2, CG_STEPS, K, 128), f32),
        D((N,)), D((N,)), D((2, N)),
        D((2, N)), D((2, N)), D((2, N)), D((2, N)), D((2, N)), D((2, N)),
        D((2, 2, ns)), D((2, 2, ns)), D((2, CG_STEPS, nc)), D((2, CG_STEPS, nc)), D((2, ns)), D((2, ns)),
    ]
    x, y, slack, dual = pl.pallas_call(
        functools.partial(kernel_body, (n_scen, n_col, B, S, R, C1, C2)),
        out_shape=(
            jax.ShapeDtypeStruct((B, C1), f32),
            jax.ShapeDtypeStruct((S, B, C2), f32),
            jax.ShapeDtypeStruct((S, B, RQ), f32),
            jax.ShapeDtypeStruct((S, B, RQ), f32),
        ),
        in_specs=[hbm, hbm, hbm, vm, vm, vm],
        out_specs=(vm, vm, vm, vm),
        scratch_shapes=scratch,
        compiler_params=pltpu.CompilerParams(
            collective_id=0, has_side_effects=True, vmem_limit_bytes=62 * 1024 * 1024),
    )(
        tech, recourse, rhs,
        cost_first.reshape(1, C1), cost_second, cone_id,
    )
    return pl.pallas_call(
        lay_out,
        out_shape=(
            jax.ShapeDtypeStruct((B, C1), f32),
            jax.ShapeDtypeStruct((B, S, C2), f32),
            jax.ShapeDtypeStruct((B, S, RQ), f32),
            jax.ShapeDtypeStruct((B, S, RQ), f32),
        ),
        in_specs=[vm, vm, vm, vm],
        out_specs=(vm, vm, vm, vm),
    )(x, y, slack, dual)


def program(tech, recourse, rhs, cost_first, cost_second, cone_id):
    n_scen = lax.axis_size("scen")
    n_col = lax.axis_size("col")
    batch = rhs.shape[0]
    fits = (
        (tech.shape[2] + recourse.shape[2]) % 256 == 0
        and tech.shape[2] % (128 * n_scen) == 0
        and tech.shape[1] % (128 * n_col) == 0
        and recourse.shape[2] % 128 == 0
        and batch % 32 == 0
        and batch <= 256
        and n_scen in (2, 4, 8, 16, 32)
        and n_col == 4
    )
    run = fused if fits else body
    return run(tech, recourse, rhs, cost_first, cost_second, cone_id)


def solution(mesh):
    placed = (
        P("scen", None, "col"),
        P("scen", None, "col"),
        P(None, "scen", None),
        P("col"),
        P("scen", "col"),
        P("scen", None),
    )
    return jax.shard_map(
        program,
        mesh=mesh,
        in_specs=placed,
        out_specs=(
            P(None, "col"),
            P(None, "scen", "col"),
            P(None, "scen", "col"),
            P(None, "scen", "col"),
        ),
        check_vma=False,
    )
```

```python
import functools

import jax
import jax.numpy as jnp
from jax import lax
from jax.experimental import pallas as pl
from jax.experimental.pallas import tpu as pltpu
from jax.sharding import PartitionSpec as P

NCONE = 128
ITERS = 3
CG_STEPS = 3
CHUNKS = 2
LAG_A = 3
LAG_B = 6
LAG_E = 7
TAIL_M = 3
TAIL_E = 7


HIGH = lax.Precision.HIGHEST


def cone_factors(lead, tail):
    norm_tail = jnp.sqrt(tail)
    inside = norm_tail <= lead
    polar = norm_tail <= -lead
    safe = jnp.where(norm_tail > 0.0, norm_tail, 1.0)
    middle = 0.5 * (lead + norm_tail)
    head = jnp.where(inside, lead, jnp.where(polar, 0.0, middle))
    scale = jnp.where(inside, 1.0, jnp.where(polar, 0.0, middle / safe))
    return (head, scale)


def body(tech, recourse, rhs, cost_first, cost_second, cone_id):
    f32 = jnp.float32
    bf16 = jnp.bfloat16
    n_scen = lax.axis_size("scen")
    n_col = lax.axis_size("col")
    batch = rhs.shape[0]
    scen_local = tech.shape[0]
    rows = tech.shape[1]
    first_cols = tech.shape[2]
    tech_flat = tech.reshape(scen_local * rows, first_cols)
    starts = jnp.concatenate(
        [jnp.ones((scen_local, 1), f32), (cone_id[:, 1:] != cone_id[:, :-1]).astype(f32)], axis=1
    )
    labels = lax.broadcasted_iota(jnp.int32, (1, 1, NCONE), 2)
    onehot = (cone_id[:, :, None] == labels).astype(f32)
    part_rows = rows // n_col
    row_start = lax.axis_index("col") * part_rows
    row_weight = 1.0 / n_col
    share_cols = first_cols // n_scen
    cost_here = lax.dynamic_slice_in_dim(
        cost_first, lax.axis_index("scen") * share_cols, share_cols, 0
    )
    first_weight = 1.0
    start_rows = starts[None]

    def couple(partial_value):
        return lax.psum_scatter(partial_value, "scen", scatter_dimension=1, tiled=True)

    def adjoint(rows_bf):
        first_part = jnp.dot(
            rows_bf.reshape(batch, scen_local * rows), tech_flat, preferred_element_type=f32
        )
        second_part = jnp.einsum("bsm,smk->bsk", rows_bf, recourse, preferred_element_type=f32)
        return (first_part, second_part)

    def local_squares(first_vec, second_vec):
        return first_weight * jnp.sum(first_vec * first_vec, axis=1) + jnp.sum(
            second_vec * second_vec, axis=(1, 2)
        )

    def total_norm(first_vec, second_vec):
        return lax.psum(local_squares(first_vec, second_vec), ("scen", "col"))

    here_rows = rhs.shape[2]
    first_sol = jnp.zeros((batch, share_cols), f32)
    second_sol = jnp.zeros((batch, scen_local, recourse.shape[2]), f32)
    slack = jnp.zeros((batch, scen_local, here_rows), f32)
    dual = jnp.zeros((batch, scen_local, here_rows), f32)
    image = jnp.zeros((batch, scen_local, here_rows), f32)
    for outer in range(ITERS):
        resid_rows = (rhs - slack - dual - image).astype(bf16)
        back_first, back_second = adjoint(resid_rows)
        res_first = couple(back_first) - cost_here[None, :]
        res_second = back_second - cost_second[None]
        res_norm = total_norm(res_first, res_second)
        dir_first, dir_second = (res_first, res_second)
        for step in range(CG_STEPS):
            dir_first_bf = lax.all_gather(dir_first.astype(bf16), "scen", axis=1, tiled=True)
            forward_partial_value = lax.dot_general(
                dir_first_bf, tech_flat, (((1,), (1,)), ((), ())), preferred_element_type=f32
            )
            forward_partial_value = forward_partial_value.reshape(batch, scen_local, rows)
            image_step = lax.psum(
                forward_partial_value
                + jnp.einsum(
                    "bsk,smk->bsm", dir_second.astype(bf16), recourse, preferred_element_type=f32
                ),
                "col",
            )
            curv_term = local_squares(dir_first, dir_second) + row_weight * jnp.sum(
                image_step * image_step, axis=(1, 2)
            )
            curv = lax.psum(curv_term, ("scen", "col"))
            alpha = res_norm / curv
            first_sol = first_sol + alpha[:, None] * dir_first
            second_sol = second_sol + alpha[:, None, None] * dir_second
            image = image + alpha[:, None, None] * image_step
            if step + 1 < CG_STEPS:
                back_first, back_second = adjoint(image_step.astype(bf16))
                res_first = res_first - alpha[:, None] * (dir_first + couple(back_first))
                res_second = res_second - alpha[:, None, None] * (dir_second + back_second)
                new_norm = total_norm(res_first, res_second)
                ratio = new_norm / res_norm
                dir_first = res_first + ratio[:, None] * dir_first
                dir_second = res_second + ratio[:, None, None] * dir_second
                res_norm = new_norm
        values = rhs - image - dual
        project_lead = jnp.einsum("bsm,smc->bsc", values * start_rows, onehot, precision=HIGH)
        project_tail = jnp.einsum(
            "bsm,smc->bsc", values * values * (1.0 - start_rows), onehot, precision=HIGH
        )
        project_lead, project_tail = (project_lead, project_tail)
        head, scale = cone_factors(project_lead, project_tail)
        head_rows = jnp.einsum("bsc,smc->bsm", head, onehot, precision=HIGH)
        scale_rows = jnp.einsum("bsc,smc->bsm", scale, onehot, precision=HIGH)
        slack = start_rows * head_rows + (1.0 - start_rows) * values * scale_rows
        dual = dual + image + slack - rhs
    first_out = lax.all_gather(first_sol, "scen", axis=1, tiled=True)
    slack_out = lax.dynamic_slice_in_dim(slack, row_start, part_rows, 2)
    dual_out = lax.dynamic_slice_in_dim(dual, row_start, part_rows, 2)
    return (first_out, second_sol, slack_out, dual_out)


def kernel_body(
    dims,
    tech_hbm, rec_hbm, rhs_hbm, cost1, cost2, cid,
    x_out, y_out, slack_out, dual_out,
    wts, wtt, g, dual, slack, onehot, part, pb, rcv_a, rcv_b, u, dz,
    px, acc, bq1, res1, dir1, sol1, xin, bk2, bq2, res2, dir2, sol2,
    sc1, sc2, uu, uv, uw,
    nres, dirn, qn, rat, alphas, rats,
    ld_t, ld_r, ld_g,
    a_s, a_r, b_s, b_r, u_s, u_r, px_s, px_r, c1_s, c1_r, c2_s, c2_r,
):
    n_scen, n_col, B, S, R, C1, C2 = dims
    f32, bf16 = jnp.float32, jnp.bfloat16
    H = CHUNKS
    RH = R // H
    N = S * H
    K = B // 2
    CB = 256
    G = K // 8
    W = 128 // (5 * G)
    SLOTS = max(N + LAG_A, LAG_B + N - TAIL_M, LAG_E + N - TAIL_E)
    TURNS = 2 * ITERS * (CG_STEPS + 1)
    ms = lax.axis_index("scen")
    mc = lax.axis_index("col")
    pair = mc + 1 - 2 * lax.rem(mc, 2)
    across = 3 - mc
    is_end = jnp.logical_or(mc == 0, mc == 3)
    is_mid = jnp.logical_or(mc == 1, mc == 2)
    mid = lax.rem((mc + 1) // 2, 2)
    lag = LAG_E + (LAG_B - LAG_E) * mid
    tail = TAIL_E + (TAIL_M - TAIL_E) * mid
    project_from = TAIL_M * mid

    def scen_peer(j):
        out = 0
        for bit in range(n_scen.bit_length() - 1):
            own = lax.rem(ms // (1 << bit), 2)
            out = out + (1 << bit) * (1 - own if j >> bit & 1 else own)
        return out

    def col_peer(j):
        return lax.rem(mc + j, n_col)

    def to_scen(src, dst, ss, rs, j):
        return pltpu.make_async_remote_copy(
            src_ref=src, dst_ref=dst, send_sem=ss, recv_sem=rs,
            device_id=(scen_peer(j), mc), device_id_type=pl.DeviceIdType.MESH)

    def to_col(src, dst, ss, rs, target):
        return pltpu.make_async_remote_copy(
            src_ref=src, dst_ref=dst, send_sem=ss, recv_sem=rs,
            device_id=(ms, target), device_id_type=pl.DeviceIdType.MESH)

    SJ = sorted(range(1, n_scen), key=lambda j: -bin(j >> 1).count("1"))
    CJ = range(1, n_col)

    def d_a(i, c):
        return to_col(pb.at[i, c], rcv_a.at[i, c], a_s.at[i, c], a_r.at[i, c], pair)

    def d_b(i, c):
        return to_col(pb.at[i, c], rcv_b.at[i, c], b_s.at[i, c], b_r.at[i, c], across)

    def d_u(i, k, c):
        return to_col(u.at[i, k, c], u.at[i, k, c], u_s.at[i, c], u_r.at[i, c], pair)

    def d_px(i, p, j):
        return to_scen(px.at[i, p, ms], px.at[i, p, ms], px_s.at[i, p, j - 1], px_r.at[i, p, j - 1], j)

    def d_c1(i, k, j):
        return to_col(sc1.at[i, k, mc], sc1.at[i, k, mc], c1_s.at[i, k, j - 1], c1_r.at[i, k, j - 1], col_peer(j))

    def d_c2(i, j):
        return to_scen(sc2.at[i, ms], sc2.at[i, ms], c2_s.at[i, j - 1], c2_r.at[i, j - 1], j)

    lane_no = lax.broadcasted_iota(jnp.int32, (8, 128), 1)
    lane_group = lane_no // W

    def pack(parts):
        out = jnp.zeros((8, 128), f32)
        for n, x in enumerate(parts):
            tot = jnp.broadcast_to(jnp.sum(x, axis=1, keepdims=True), (K, 128))
            for k in range(G):
                out = jnp.where(lane_group == n * G + k, tot[8 * k:8 * k + 8], out)
        return out

    def unpack(p):
        return [jnp.concatenate(
            [jnp.broadcast_to(
                jnp.sum(jnp.where(lane_no == W * (n * G + k), p, 0.0), axis=1, keepdims=True), (8, 128))
             for k in range(G)], axis=0) for n in range(5)]

    def lanes(x):
        out = x[:, 0:128]
        for k in range(1, x.shape[1] // 128):
            out = out + x[:, 128 * k:128 * k + 128]
        return out

    def rows_of(c):
        return c // H, pl.ds(pl.multiple_of(lax.rem(c, H) * RH, RH), RH)

    def load_t(c):
        s, rows = rows_of(c)
        return pltpu.make_async_copy(tech_hbm.at[s, rows, :], wts.at[c, :, pl.ds(0, C1)], ld_t.at[c])

    def load_r(c):
        s, rows = rows_of(c)
        return pltpu.make_async_copy(rec_hbm.at[s, rows, :], wts.at[c, :, pl.ds(C1, C2)], ld_r.at[c])

    def load_g(i, c):
        s, rows = rows_of(c)
        return pltpu.make_async_copy(rhs_hbm.at[pl.ds(i * K, K), s, rows], g.at[i, c], ld_g.at[i, c])

    def each(n, f):
        def one(c, carry):
            f(c)
            return carry
        lax.fori_loop(0, n, one, 0)

    def load_all(c):
        load_g(0, c).start()
        load_g(1, c).start()
        load_t(c).start()
        load_r(c).start()

    each(N, load_all)

    barrier = pltpu.get_barrier_semaphore()
    for j in SJ:
        pl.semaphore_signal(barrier, inc=1, device_id=(scen_peer(j), mc), device_id_type=pl.DeviceIdType.MESH)
    for j in CJ:
        pl.semaphore_signal(barrier, inc=1, device_id=(ms, col_peer(j)), device_id_type=pl.DeviceIdType.MESH)

    for ref in (bq1, dir1, sol1, bq2, dir2, sol2, uu, uv, uw, nres, dirn, qn, rat, dual, u, acc, bk2):
        ref[...] = jnp.zeros_like(ref)

    def init_cones(s):
        ids = cid[pl.ds(s, 1), :]
        onehot[s] = (lax.broadcasted_iota(jnp.int32, (NCONE, R), 0) == ids).astype(f32).astype(bf16)

    each(S, init_cones)

    def add_back(i, s, f):
        acc[i] = acc[i] + f[:, 0:C1]
        bk2[i, s] = bk2[i, s] + f[:, C1:C1 + C2]

    def back(i, c, z):
        add_back(i, c // H, jnp.dot(z, wts[c], preferred_element_type=f32))

    def first_back(c):
        load_g(0, c).wait()
        load_g(1, c).wait()
        load_t(c).wait()
        load_r(c).wait()
        z = jnp.concatenate([g[0, c], g[1, c]], axis=0).astype(bf16)
        f = jnp.dot(z, wts[c], preferred_element_type=f32)
        add_back(0, c // H, f[0:K])
        add_back(1, c // H, f[K:2 * K])
        for j in range((C1 + C2) // CB):
            cols = slice(j * CB, (j + 1) * CB)
            wtt[c, cols, :] = wts[c, :, cols].T

    each(N, first_back)
    pl.semaphore_wait(barrier, n_scen + n_col - 2)

    def send_first(i, p):
        px[i, p, ms] = acc[i].astype(bf16)
        for j in SJ:
            d_px(i, p, j).start()

    def take_first(i, p):
        for j in SJ:
            d_px(i, p, j).wait_recv()
        tot = px[i, p, 0].astype(f32)
        for k in range(1, n_scen):
            tot = tot + px[i, p, k].astype(f32)
        for j in SJ:
            d_px(i, p, j).wait_send()
        return tot

    def send_norms(i, k):
        r1 = res1[i]
        sq = lanes(r1 * r1) * (1.0 / n_scen)
        cr = lanes(r1 * dir1[i]) * (1.0 / n_scen)
        for s in range(S):
            r2 = res2[i, s]
            sq = sq + lanes(r2 * r2)
            cr = cr + lanes(r2 * dir2[i, s])
        sc1[i, k, mc] = pack([sq, cr])
        for j in CJ:
            d_c1(i, k, j).start()

    def restart(i):
        r1 = take_first(i, 1) - cost1[...]
        res1[i] = r1
        xin[i] = r1.astype(bf16)
        for s in range(S):
            res2[i, s] = bk2[i, s] - cost2[s:s + 1, :]

    send_first(0, 1)
    send_first(1, 1)
    restart(0)

    def front(i, c):
        x = jnp.concatenate([xin[i], res2[i, c // H].astype(bf16)], axis=1)
        return jnp.dot(x, wtt[c], preferred_element_type=f32)

    def relay(i, c):
        d_a(i, c).wait_recv()
        pb[i, c] = (part[c] + rcv_a[i, c].astype(f32)).astype(bf16)
        d_b(i, c).start()

    def finish_rows(i, k, c):
        @pl.when(is_end)
        def _():
            d_u(i, k, c).wait_recv()

        @pl.when(is_mid)
        def _():
            d_b(i, c).wait_recv()
            u[i, k, c] = (pb[i, c].astype(f32) + rcv_b[i, c].astype(f32)).astype(bf16)
            d_u(i, k, c).start()

        v = u[i, k, c].astype(f32)
        before = u[i, lax.rem(k + CG_STEPS - 1, CG_STEPS), c].astype(f32)
        earlier = u[i, lax.rem(k + CG_STEPS - 2, CG_STEPS), c].astype(f32)
        uu[i] = uu[i] + lanes(v * v)
        uv[i] = uv[i] + lanes(v * before)
        uw[i] = uw[i] + lanes(v * earlier)

    def send_scalars(i, k):
        total = pack([jnp.zeros((K, 128), f32)] * 2 + [uu[i], uv[i], uw[i]])
        for j in CJ:
            d_c1(i, k, j).wait_recv()
        for m in range(n_col):
            total = total + sc1[i, k, m]
        for j in CJ:
            d_c1(i, k, j).wait_send()
        sc2[i, ms] = total
        for j in SJ:
            d_c2(i, j).start()

    def finish_scalars(i, k):
        for j in SJ:
            d_c2(i, j).wait_recv()
        total = sc2[i, 0]
        for m in range(1, n_scen):
            total = total + sc2[i, m]
        for j in SJ:
            d_c2(i, j).wait_send()
        s0, s1, s2, s3, s4 = unpack(total)
        r = jnp.where(k == 0, 0.0, s0 / nres[i])
        dn = s0 + r * (2.0 * s1 + r * dirn[i])
        qs = s2 + r * (2.0 * (s3 + rat[i] * s4) + r * qn[i])
        nres[i] = s0
        dirn[i] = dn
        qn[i] = qs
        rat[i] = r
        rats[i, k] = r
        a = s0 / (dn + qs)
        alphas[i, k] = a
        r, a = r[:, 0:1], a[:, 0:1]
        d1 = res1[i] + r * dir1[i]
        dir1[i] = d1
        sol1[i] = sol1[i] + a * d1
        for s in range(S):
            d2 = res2[i, s] + r * dir2[i, s]
            dir2[i, s] = d2
            sol2[i, s] = sol2[i, s] + a * d2

    def next_residual(i, k):
        r, a = rats[i, k][:, 0:1], alphas[i, k][:, 0:1]
        q1 = take_first(i, lax.rem(k, 2)) + r * bq1[i]
        bq1[i] = q1
        r1 = res1[i] - a * (dir1[i] + q1)
        res1[i] = r1
        xin[i] = r1.astype(bf16)
        for s in range(S):
            q2 = bk2[i, s] + r * bq2[i, s]
            bq2[i, s] = q2
            res2[i, s] = res2[i, s] - a * (dir2[i, s] + q2)

    def all_sent(i, k):
        @pl.when(is_end)
        def _():
            each(N, lambda c: d_a(i, c).wait_send())

        @pl.when(is_mid)
        def _():
            def one(c):
                d_b(i, c).wait_send()
                d_u(i, k, c).wait_send()

            each(N, one)

    def split(x):
        hi = x.astype(bf16)
        return [hi, (x - hi.astype(f32)).astype(bf16)]

    def project(i, s):
        c2 = alphas[i, 2]
        c1 = alphas[i, 1] + rats[i, 2] * c2
        c0 = alphas[i, 0] + rats[i, 1] * c1
        c0, c1, c2 = c0[:, 0:1], c1[:, 0:1], c2[:, 0:1]
        ids = cid[pl.ds(s, 1), :]
        first = lax.broadcasted_iota(jnp.int32, (1, R), 1) == 0
        st = jnp.where(jnp.logical_or(first, ids != pltpu.roll(ids, 1, 1)), 1.0, 0.0)
        pieces = []
        for h in range(H):
            c = s * H + h
            piece = g[i, c] - (c0 * u[i, 0, c].astype(f32) + c1 * u[i, 1, c].astype(f32)
                               + c2 * u[i, 2, c].astype(f32))
            g[i, c] = piece
            pieces.append(piece)
        gs = jnp.concatenate(pieces, axis=1)
        v = gs - jnp.concatenate([dual[i, s * H + h] for h in range(H)], axis=1)
        lead_v = v * st
        tail_v = v * v * (1.0 - st)
        stack = jnp.concatenate(split(lead_v) + split(tail_v), axis=0)
        sums = lax.dot_general(stack, onehot[s], (((1,), (1,)), ((), ())), preferred_element_type=f32)
        lead = sums[0:K] + sums[K:2 * K]
        tail = sums[2 * K:3 * K] + sums[3 * K:4 * K]
        head, scale = cone_factors(lead, tail)
        stack2 = jnp.concatenate(split(head) + split(scale), axis=0)
        outs = jnp.dot(stack2, onehot[s], preferred_element_type=f32)
        head_rows = outs[0:K] + outs[K:2 * K]
        scale_rows = outs[2 * K:3 * K] + outs[3 * K:4 * K]
        sl = st * head_rows + (1.0 - st) * v * scale_rows
        du = sl - v
        d = (gs - sl - du).astype(bf16)
        for h in range(H):
            cols = slice(h * RH, (h + 1) * RH)
            slack[i, s * H + h] = sl[:, cols]
            dual[i, s * H + h] = du[:, cols]
            dz[s * H + h] = d[:, cols]

    def turn(t, carry):
        a = lax.rem(t, 2)
        b = 1 - a
        ka = lax.rem(t // 2, CG_STEPS + 1)
        kb = lax.rem((t + 2 * CG_STEPS + 1) // 2, CG_STEPS + 1)
        run_a, run_b = ka < CG_STEPS, kb < CG_STEPS
        back_a, back_b = ka < CG_STEPS - 1, kb < CG_STEPS - 1
        acc[a] = jnp.zeros((K, C1), f32)
        bk2[a] = jnp.zeros((S, K, C2), f32)
        uu[a] = jnp.zeros((K, 128), f32)
        uv[a] = jnp.zeros((K, 128), f32)
        uw[a] = jnp.zeros((K, 128), f32)

        def keep_front(c):
            p = front(a, c)
            part[c] = p
            pb[a, c] = p.astype(bf16)

        @pl.when(run_a)
        def _():
            keep_front(0)

            @pl.when(is_end)
            def _():
                d_a(a, 0).start()

        def slot(k):
            @pl.when(jnp.logical_and(run_a, k == 1))
            def _():
                send_norms(a, ka)

            @pl.when(jnp.logical_and(jnp.logical_not(run_a), jnp.logical_and(k >= project_from, k < project_from + S)))
            def _():
                project(a, k - project_from)

            ends_tail = k == tail - 1
            in_tail = jnp.logical_and(run_b, k < tail)
            in_front = jnp.logical_and(run_a, k + 1 < N)
            both = jnp.logical_and(jnp.logical_and(in_front, in_tail), back_b)
            c = jnp.minimum(N - tail + k, N - 1)

            @pl.when(in_tail)
            def _():
                finish_rows(b, kb, c)

                @pl.when(ends_tail)
                def _():
                    send_scalars(b, kb)

            @pl.when(both)
            def _():
                keep_front(k + 1)
                back(b, c, u[b, kb, c])

            @pl.when(jnp.logical_and(in_front, jnp.logical_not(both)))
            def _():
                keep_front(k + 1)

            @pl.when(jnp.logical_and(jnp.logical_and(in_tail, back_b), jnp.logical_not(both)))
            def _():
                back(b, c, u[b, kb, c])

            @pl.when(jnp.logical_and(in_front, is_end))
            def _():
                d_a(a, k + 1).start()

            @pl.when(jnp.logical_and(jnp.logical_and(in_tail, back_b), ends_tail))
            def _():
                send_first(b, lax.rem(kb, 2))

            @pl.when(jnp.logical_and(jnp.logical_and(run_a, is_mid), jnp.logical_and(k >= LAG_A, k < LAG_A + N)))
            def _():
                relay(a, k - LAG_A)

            @pl.when(jnp.logical_and(run_a, jnp.logical_and(k >= lag, k < lag + N - tail)))
            def _():
                c = k - lag
                finish_rows(a, ka, c)

                @pl.when(back_a)
                def _():
                    back(a, c, u[a, ka, c])

        each(SLOTS, slot)

        @pl.when(ka == CG_STEPS)
        def _():
            @pl.when(t < TURNS - 2)
            def _():
                def pair_back(n):
                    back(a, 2 * n, dz[2 * n])
                    back(a, 2 * n + 1, dz[2 * n + 1])

                each(N // 2, pair_back)
                send_first(a, 1)

        @pl.when(run_b)
        def _():
            finish_scalars(b, kb)
            all_sent(b, kb)

        @pl.when(back_b)
        def _():
            next_residual(b, kb)

        @pl.when(jnp.logical_and(kb == CG_STEPS, t < TURNS - 1))
        def _():
            restart(b)

        return carry

    lax.fori_loop(0, TURNS, turn, 0)

    RQ = R // n_col
    own = mc * RQ // RH
    here = pl.ds(pl.multiple_of(lax.rem(mc * RQ, RH), 128), RQ)
    for i in range(2):
        rows = slice(i * K, (i + 1) * K)
        x_out[rows, :] = sol1[i]
        for s in range(S):
            y_out[s, rows, :] = sol2[i, s]
            slack_out[s, rows, :] = slack[i, s * H + own, :, here]
            dual_out[s, rows, :] = dual[i, s * H + own, :, here]


def lay_out(x, y, slack, dual, x_out, y_out, slack_out, dual_out):
    x_out[...] = x[...]
    for s in range(y.shape[0]):
        y_out[:, s, :] = y[s]
        slack_out[:, s, :] = slack[s]
        dual_out[:, s, :] = dual[s]


def fused(tech, recourse, rhs, cost_first, cost_second, cone_id):
    f32, bf16 = jnp.float32, jnp.bfloat16
    n_scen = lax.axis_size("scen")
    n_col = lax.axis_size("col")
    B = rhs.shape[0]
    S, R, C1 = tech.shape
    C2 = recourse.shape[2]
    RQ = R // n_col
    RH = R // CHUNKS
    N = S * CHUNKS
    K = B // 2
    vm = pl.BlockSpec(memory_space=pltpu.VMEM)
    hbm = pl.BlockSpec(memory_space=pl.ANY)
    V = pltpu.VMEM
    D = pltpu.SemaphoreType.DMA
    ns, nc = n_scen - 1, n_col - 1
    rows = lambda dt: V((2, N, K, RH), dt)
    one = V((2, K, C1), f32)
    two = V((2, S, K, C2), f32)
    num = V((2, K, 128), f32)
    scratch = [
        V((N, RH, C1 + C2), bf16), V((N, C1 + C2, RH), bf16),
        rows(f32), rows(f32), rows(f32), V((S, NCONE, R), bf16), V((N, K, RH), f32),
        rows(bf16), rows(bf16), rows(bf16), V((2, CG_STEPS, N, K, RH), bf16), V((N, K, RH), bf16),
        V((2, 2, n_scen, K, C1), bf16), one, one, one, one, one, V((2, K, C1), bf16),
        two, two, two, two, two,
        V((2, CG_STEPS, n_col, 8, 128), f32), V((2, n_scen, 8, 128), f32), num, num, num,
        num, num, num, num, V((2, CG_STEPS, K, 128), f32), V((2, CG_STEPS, K, 128), f32),
        D((N,)), D((N,)), D((2, N)),
        D((2, N)), D((2, N)), D((2, N)), D((2, N)), D((2, N)), D((2, N)),
        D((2, 2, ns)), D((2, 2, ns)), D((2, CG_STEPS, nc)), D((2, CG_STEPS, nc)), D((2, ns)), D((2, ns)),
    ]
    x, y, slack, dual = pl.pallas_call(
        functools.partial(kernel_body, (n_scen, n_col, B, S, R, C1, C2)),
        out_shape=(
            jax.ShapeDtypeStruct((B, C1), f32),
            jax.ShapeDtypeStruct((S, B, C2), f32),
            jax.ShapeDtypeStruct((S, B, RQ), f32),
            jax.ShapeDtypeStruct((S, B, RQ), f32),
        ),
        in_specs=[hbm, hbm, hbm, vm, vm, vm],
        out_specs=(vm, vm, vm, vm),
        scratch_shapes=scratch,
        compiler_params=pltpu.CompilerParams(
            collective_id=0, has_side_effects=True, vmem_limit_bytes=62 * 1024 * 1024),
    )(
        tech, recourse, rhs,
        cost_first.reshape(1, C1), cost_second, cone_id,
    )
    return pl.pallas_call(
        lay_out,
        out_shape=(
            jax.ShapeDtypeStruct((B, C1), f32),
            jax.ShapeDtypeStruct((B, S, C2), f32),
            jax.ShapeDtypeStruct((B, S, RQ), f32),
            jax.ShapeDtypeStruct((B, S, RQ), f32),
        ),
        in_specs=[vm, vm, vm, vm],
        out_specs=(vm, vm, vm, vm),
    )(x, y, slack, dual)


def program(tech, recourse, rhs, cost_first, cost_second, cone_id):
    n_scen = lax.axis_size("scen")
    n_col = lax.axis_size("col")
    batch = rhs.shape[0]
    fits = (
        (tech.shape[2] + recourse.shape[2]) % 256 == 0
        and tech.shape[2] % (128 * n_scen) == 0
        and tech.shape[1] % (128 * n_col) == 0
        and recourse.shape[2] % 128 == 0
        and batch % 32 == 0
        and batch <= 256
        and n_scen in (2, 4, 8, 16, 32)
        and n_col == 4
    )
    run = fused if fits else body
    return run(tech, recourse, rhs, cost_first, cost_second, cone_id)


def solution(mesh):
    placed = (
        P("scen", None, "col"),
        P("scen", None, "col"),
        P(None, "scen", None),
        P("col"),
        P("scen", "col"),
        P("scen", None),
    )
    return jax.shard_map(
        program,
        mesh=mesh,
        in_specs=placed,
        out_specs=(
            P(None, "col"),
            P(None, "scen", "col"),
            P(None, "scen", "col"),
            P(None, "scen", "col"),
        ),
        check_vma=False,
    )
```
